32 devices in a mesh: aa: 8 (over y, x, core), ba: 4 (over z).
Axes of the slice: x: 2, y: 2, z: 4, core: 2. Of those that a mesh axis runs over, the one named last changes fastest.
Arguments:
- queries: bfloat16 [4, 128, 8192], P('ba', None, 'aa'), may hold values from -10 to 10
- new_kv: bfloat16 [4, 128, 2, 512], P('ba', 'aa'), may hold values from -4 to 4
- pool: bfloat16 [4, 64, 32, 2, 512], P('ba', 'aa'), may hold values from -4 to 4
- page_table: int32 [4, 32], P('ba', 'aa'), may hold values from 0 to 7, as said below
- ctx_len: int32 [4, 8], P('ba', 'aa'), may hold values from 1 to 128, as said below
- move_page: int32 [4, 24], P('ba', 'aa'), may hold values from 0 to 7, as said below
- move_dest: int32 [4, 24], P('ba', 'aa'), may hold values from 0 to 3, as said below
- append_page: int32 [4, 8], P('ba', 'aa'), may hold values from 0 to 7
Outputs:
- attended: bfloat16 [4, 128, 8192], P('ba', None, 'aa')
- pool_out: bfloat16 [4, 64, 32, 2, 512], P('ba', 'aa')
The draws below stay inside these ranges and needn't reach their ends.
Inputs may be any that keep to these rules, and one draw needn't show every extreme that they name: `page_table`: the entries of one device are distinct pages of its pool and differ from its leaving pages and its append page. `ctx_len`: for each instance some index of aa holds exactly 128 live rows. `move_page`: the 3 entries of one device are distinct pages of its pool. `move_dest`: A device never names its own instance and names any one instance at most 2 times; for each index of aa one instance is named exactly 2 times by the device of every other instance.
All inputs are finite; a program needn't handle non-finite values.
Results may differ from the reference program's by a relative error of at most 0.0017.
Values may be sent and summed in bfloat16 or wider, within the bound.
A program may use at most 64 MiB of HBM per device.

```python
import math
import jax
import jax.numpy as jnp
from jax import lax

HEADS = 64
KV_HEADS = 4
HEAD_DIM = 128
PAGE = 32
MOST = 2
NEW_ROWS = 128
TABLE = 4
GROUP = 16
INSTANCES = 4
MOVES = 3
POOL = 8
NEW_DEV = 16
N_AA = 8


def draw_new_kv(key, part):
    out_shape = (INSTANCES, NEW_ROWS, 2, KV_HEADS * HEAD_DIM)
    values = jnp.clip(jax.random.normal(jax.random.fold_in(key, 71), out_shape, jnp.float32), -4.0, 4.0)
    return values.astype(jnp.bfloat16)


def draw_queries(key, part):
    out_shape = (INSTANCES, NEW_ROWS, HEADS * HEAD_DIM)
    drawn = 2.5 * jax.random.normal(jax.random.fold_in(key, 75), out_shape, jnp.float32)
    return jnp.clip(drawn, -10.0, 10.0).astype(jnp.bfloat16)


def shuffle_pages(sub_key):
    return jax.random.permutation(sub_key, POOL).astype(jnp.int32)


def page_lists(key):
    sub_keys = jax.random.split(jax.random.fold_in(key, 31), INSTANCES * N_AA)
    orders = jax.vmap(shuffle_pages)(sub_keys)
    return orders.reshape(INSTANCES, N_AA, POOL)


def draw_page_table(key, part):
    return page_lists(key)[:, :, :TABLE].reshape(INSTANCES, N_AA * TABLE)


def draw_move_page(key, part):
    return page_lists(key)[:, :, TABLE:TABLE + MOVES].reshape(INSTANCES, N_AA * MOVES)


def draw_append_page(key, part):
    return page_lists(key)[:, :, TABLE + MOVES]


def shuffle_slots(sub_key):
    return jax.random.permutation(sub_key, (INSTANCES - 1) * MOST).astype(jnp.int32)


def draw_move_dest(key, part):
    seeded = jax.random.fold_in(key, 37)
    option_count = (INSTANCES - 1) * MOST
    busiest = jax.random.randint(jax.random.fold_in(seeded, 1), (N_AA,), 0, INSTANCES)
    source = jnp.arange(INSTANCES)[:, None]
    candidate = (source + 1 + jnp.arange(option_count)[None, :] // MOST) % INSTANCES
    sub_keys = jax.random.split(jax.random.fold_in(seeded, 2), INSTANCES * N_AA)
    scores = jax.vmap(shuffle_slots)(sub_keys).reshape(INSTANCES, N_AA, option_count)
    forced = candidate[:, None, :] == busiest[None, :, None]
    priority = jnp.where(forced, scores + option_count, scores)
    picked = lax.top_k(priority, MOVES)[1]
    spread = jnp.broadcast_to(candidate[:, None, :], priority.shape)
    chosen_dest = jnp.take_along_axis(spread, picked, axis=-1)
    return chosen_dest.reshape(INSTANCES, N_AA * MOVES).astype(jnp.int32)


def draw_ctx_len(key, part):
    seeded = jax.random.fold_in(key, 41)
    full_rows = TABLE * PAGE
    lengths = jax.random.randint(jax.random.fold_in(seeded, 1), (INSTANCES, N_AA), 1, full_rows + 1)
    full_index = jax.random.randint(jax.random.fold_in(seeded, 2), (INSTANCES,), 0, N_AA)
    hit_full = jnp.arange(N_AA)[None, :] == full_index[:, None]
    return jnp.where(hit_full, full_rows, lengths).astype(jnp.int32)


def shard_levels(own_key, dims, shards, smallest, top_value):
    level = 1.0
    for dim, parts in shards:
        steps = jax.random.uniform(jax.random.fold_in(jax.random.fold_in(own_key, 6), dim), (parts,), jnp.float32, smallest / len(shards), top_value / len(shards))
        level = level * jnp.repeat(jnp.exp(steps), dims[dim] // parts).reshape((-1,) + (1,) * (len(dims) - 1 - dim))
    return level


def scatter_about(key, shape, scale, most, cuts=(), kind=jnp.bfloat16):
    level = shard_levels(key, shape, cuts, -0.22, 0.18) if cuts else 1.0
    values = jax.random.normal(key, shape, jnp.float32) * scale * level
    return jnp.minimum(jnp.maximum(values, -most), most).astype(kind)


def setup_inputs(seed: int = 0) -> dict:
    key_list = jax.random.split(jax.random.key(seed), 9)
    queries = draw_queries(jax.random.fold_in(key_list[8], 71), 0)
    new_kv = draw_new_kv(jax.random.fold_in(key_list[8], 71), 0)
    pool = scatter_about(key_list[2], (INSTANCES, N_AA * POOL, PAGE, 2, KV_HEADS * HEAD_DIM), 1.0, 4.0, ((0, 4), (1, 8)))
    page_table = draw_page_table(jax.random.fold_in(key_list[8], 71), 0)
    ctx_len = draw_ctx_len(jax.random.fold_in(key_list[8], 71), 0)
    move_page = draw_move_page(jax.random.fold_in(key_list[8], 71), 0)
    move_dest = draw_move_dest(jax.random.fold_in(key_list[8], 71), 0)
    append_page = draw_append_page(jax.random.fold_in(key_list[8], 71), 0)
    return dict(queries=queries, new_kv=new_kv, pool=pool, page_table=page_table, ctx_len=ctx_len, move_page=move_page, move_dest=move_dest, append_page=append_page)


def pick_pages(pages, page_ids):
    return jnp.take(pages, page_ids.astype(jnp.int32), axis=0)

def place_rows(pages, fresh_rows, page_id):
    start = page_id.astype(jnp.int32)
    zero = jnp.zeros((), jnp.int32)
    return lax.dynamic_update_slice(pages, fresh_rows[None], (start, zero, zero, zero))

def attention(query_rows, key_rows, visible):
    query_heads = query_rows.astype(jnp.float32).reshape(NEW_ROWS, KV_HEADS, GROUP, HEAD_DIM).transpose(1, 0, 2, 3)
    head_keys = key_rows[:, 0].astype(jnp.float32).reshape(-1, KV_HEADS, HEAD_DIM).transpose(1, 0, 2)
    head_values = key_rows[:, 1].astype(jnp.float32).reshape(-1, KV_HEADS, HEAD_DIM).transpose(1, 0, 2)

    def one_head(operands):
        head_query, key_block, value_block = operands
        scores = jnp.einsum('qgd,rd->qgr', head_query, key_block) / math.sqrt(HEAD_DIM)
        scores = jnp.where(visible[:, None, :], scores, -jnp.inf)
        row_top = lax.optimization_barrier(jnp.max(scores, axis=-1, keepdims=True))
        weights = jnp.exp(scores - row_top)
        row_total = lax.optimization_barrier(jnp.sum(weights, axis=-1))
        return jnp.einsum('qgr,rd->qgd', weights, value_block, precision=lax.Precision.HIGHEST) / row_total[..., None]
    outputs = lax.map(one_head, (query_heads, head_keys, head_values))
    return outputs.transpose(1, 0, 2, 3).reshape(NEW_ROWS, HEADS * HEAD_DIM).astype(jnp.bfloat16)

def reference(queries, new_kv, pool, page_table, ctx_len, move_page, move_dest, append_page):
    kv_width = KV_HEADS * HEAD_DIM
    pool_pages = pool.reshape(INSTANCES, N_AA, POOL, PAGE, 2, kv_width)
    tables = page_table.reshape(INSTANCES, N_AA, TABLE)
    moved_ids = move_page.reshape(INSTANCES, N_AA, MOVES)
    targets = move_dest.reshape(INSTANCES, N_AA, MOVES)
    counter = jnp.arange(MOVES, dtype=jnp.int32)
    earlier = counter[None, :] < counter[:, None]
    same_target = targets[..., :, None] == targets[..., None, :]
    ranks = lax.optimization_barrier(jnp.sum(same_target & earlier, axis=-1)).astype(jnp.int32)
    pick_all = jax.vmap(jax.vmap(pick_pages))
    slot_numbers = jnp.arange(MOST, dtype=jnp.int32)
    row_offsets = jnp.arange(TABLE * PAGE, dtype=jnp.int32)
    causal = jnp.arange(NEW_ROWS, dtype=jnp.int32)[None, :] <= jnp.arange(NEW_ROWS, dtype=jnp.int32)[:, None]

    def serve_instance(target):
        slot_hit = (targets == target)[..., None] & (ranks[..., None] == slot_numbers)
        page_ids = lax.optimization_barrier(jnp.sum(jnp.where(slot_hit, moved_ids[..., None], 0), axis=2)).astype(jnp.int32)
        arrived = jnp.any(slot_hit, axis=2)
        moved_rows = pick_all(pool_pages, page_ids).reshape(-1, 2, kv_width)
        moved_live = jnp.broadcast_to(arrived[..., None], (INSTANCES, N_AA, MOST, PAGE)).reshape(-1)
        own_pages = lax.dynamic_index_in_dim(pool_pages, target, 0, keepdims=False)
        own_table = lax.dynamic_index_in_dim(tables, target, 0, keepdims=False)
        own_rows = jax.vmap(pick_pages)(own_pages, own_table).reshape(-1, 2, kv_width)
        lengths = lax.dynamic_index_in_dim(ctx_len, target, 0, keepdims=False)
        own_live = (row_offsets[None, :] < lengths[:, None]).reshape(-1)
        fresh_rows = lax.dynamic_index_in_dim(new_kv, target, 0, keepdims=False)
        key_rows = jnp.concatenate([own_rows, moved_rows, fresh_rows], axis=0)
        visible = jnp.concatenate([jnp.broadcast_to(own_live[None, :], (NEW_ROWS, own_live.shape[0])), jnp.broadcast_to(moved_live[None, :], (NEW_ROWS, moved_live.shape[0])), causal], axis=1)
        query_rows = lax.dynamic_index_in_dim(queries, target, 0, keepdims=False)
        return attention(query_rows, key_rows, visible)
    attended = lax.map(serve_instance, jnp.arange(INSTANCES, dtype=jnp.int32))
    fresh_all = new_kv.reshape(INSTANCES, N_AA, NEW_DEV, 2, kv_width)
    updated = jax.vmap(jax.vmap(place_rows))(pool_pages, fresh_all, append_page)
    return (attended, updated.reshape(pool.shape))
```

```python
import functools
import math

import jax
import jax.numpy as jnp
from jax import lax
from jax.experimental import pallas as pl
from jax.experimental.pallas import tpu as pltpu
from jax.sharding import PartitionSpec as P

HEAD_DIM = 128
MOST = 2
LANES = 128
BLOCK = 256
NEG_LARGE = -1e30
MESH = pl.DeviceIdType.MESH


def kernel(
    n_inst, n_aa, kv_heads,
    table_ref, len_ref, page_ref, dest_ref, q_hbm, pool_hbm, fresh_hbm,
    out_ref,
    q_ref, pool_ref, fresh_ref,
    st_mov, st_rn, st_near, st_fwd, raw, raw_far, kv_mov, kv_rn, metas,
    run_max, run_sum, run_out, q_turned,
    s_load, s_all, r_rn, r_mov, r_raw, r_far, r_row, r_meta,
):
    b = lax.axis_index("ba")
    a = lax.axis_index("aa")
    share = n_aa // kv_heads
    mine, member = a // share, a % share
    half = n_inst // 2
    side = b // half
    base = side * half
    pos = b - base
    hub = half - 1 + side
    far_hub = half - side
    far_base = half - base
    is_hub = b == hub
    reach = (1 - side) * (half - 1 - pos) + side * pos
    near_count = half - 1
    far_count = half
    table = table_ref.shape[1]
    moves = page_ref.shape[1]
    page_rows = pool_ref.shape[1]
    fresh = fresh_ref.shape[0]
    queries = q_ref.shape[0]
    heads = q_ref.shape[1] // HEAD_DIM
    bits = (n_inst - 1).bit_length()

    def near(k):
        return base + lax.rem(pos + k + half, half)

    def flip(j):
        to = mine
        bit = 1
        while bit <= j:
            if j & bit:
                to = to + bit - 2 * bit * (mine // bit % 2)
            bit *= 2
        return to

    def at_head(j):
        return flip(j) * share + member

    def peer(k):
        return mine * share + lax.rem(member + k, share)

    pool_load = pltpu.make_async_copy(pool_hbm, pool_ref, s_load.at[0])
    pool_load.start()
    q_load = pltpu.make_async_copy(q_hbm, q_ref, s_load.at[1])
    q_load.start()
    fresh_load = pltpu.make_async_copy(fresh_hbm, fresh_ref, s_load.at[2])
    fresh_load.start()

    barrier = pltpu.get_barrier_semaphore()
    partners = [(b, at_head(j)) for j in range(1, kv_heads)]
    partners += [(b, peer(k)) for k in range(1, share)]
    partners += [(near(k), a) for k in range(1, half)]
    partners += [(far_base + f, a) for f in range(half)]
    for ba, aa in partners:
        pl.semaphore_signal(barrier, inc=1, device_id={"ba": ba, "aa": aa}, device_id_type=MESH)

    def columns_of(h):
        return slice(h * HEAD_DIM, (h + 1) * HEAD_DIM)

    code = len_ref[0, 0]
    for i in range(moves):
        code = code * (1 << bits) + dest_ref[0, i]
    metas[0, 0, 0] = jnp.full((1, LANES), code, jnp.int32)

    pool_load.wait()
    for h in range(kv_heads):
        for i in range(moves):
            for w in range(2):
                st_mov[h, i, w] = pool_ref[page_ref[0, i], :, w, columns_of(h)]

    def remote(src, dst, ss, rs, ba, aa):
        return pltpu.make_async_remote_copy(
            src_ref=src, dst_ref=dst, send_sem=ss, recv_sem=rs,
            device_id={"ba": ba, "aa": aa}, device_id_type=MESH,
        )

    sent, hub_sent = [], []

    def start(src, dst, rs, ba, aa, kept=sent, spot=None):
        c = remote(src, dst, s_all.at[len(sent) + len(hub_sent)], rs, ba, aa)
        c.start()
        kept.append((spot or src, len(sent) + len(hub_sent)))

    def arrived(slot, rs):
        remote(slot, slot, s_all.at[0], rs, b, a).wait_recv()

    def shifted(row, count):
        return lax.shift_right_logical(row, jnp.full(row.shape, count, jnp.int32))

    def dests_of(row):
        low = jnp.full(row.shape, (1 << bits) - 1, jnp.int32)
        return [lax.bitwise_and(shifted(row, bits * (moves - 1 - i)), low) for i in range(moves)]

    def picks(row, target):
        seen = jnp.zeros((1, LANES), jnp.int32)
        chosen = [[] for _ in range(MOST)]
        for dest in dests_of(row):
            hit = (dest == target).astype(jnp.int32)
            for m in range(MOST):
                chosen[m].append(hit * (seen == m).astype(jnp.int32))
            seen = seen + hit
        return chosen

    def select(pages, row, target, into):
        chosen = picks(row, target)
        for m in range(MOST):
            masks = [jnp.broadcast_to(c.astype(jnp.float32), (page_rows, LANES)).astype(jnp.bfloat16) for c in chosen[m]]
            for w in range(2):
                total = pages[0, w] * masks[0]
                for i in range(1, moves):
                    total = total + pages[i, w] * masks[i]
                into[w, m * page_rows:(m + 1) * page_rows, :] = total

    def to_peers(buf, sems, *at):
        for k in range(1, share):
            lead, tail = at[:-1], at[-1:]
            there = (*lead, share - k, *tail)
            here = (*lead, 0, *tail)
            start(buf.at[here], buf.at[there], sems.at[there], b, peer(k))

    def send_moved(j):
        own = st_mov.at[mine] if j == 0 else raw.at[j]
        if j:
            arrived(raw.at[j], r_raw.at[j])
        start(own, raw_far.at[reach, j], r_far.at[reach, j], far_hub, a)
        if half > 1:
            if j:
                arrived(metas.at[0, 0, j], r_row.at[j])
            row = metas[0, 0, j]
            for k in range(1, half):
                select(own, row, near(k), st_near.at[k - 1, j])
                start(st_near.at[k - 1, j], kv_mov.at[k - 1, 0, j], r_mov.at[k - 1, 0, j], near(k), a)
        elif j:
            arrived(metas.at[0, 0, j], r_row.at[j])

    pl.semaphore_wait(barrier, len(partners))

    start(st_mov.at[mine], raw_far.at[reach, 0], r_far.at[reach, 0], far_hub, a)
    for j in range(1, kv_heads):
        start(metas.at[0, 0, 0], metas.at[0, 0, j], r_row.at[j], b, at_head(j))
    for j in range(1, kv_heads):
        start(st_mov.at[flip(j)], raw.at[j], r_raw.at[j], b, at_head(j))
    for k in range(1, half):
        select(st_mov.at[mine], metas[0, 0, 0], near(k), st_near.at[k - 1, 0])
        start(st_near.at[k - 1, 0], kv_mov.at[k - 1, 0, 0], r_mov.at[k - 1, 0, 0], near(k), a)

    fresh_load.wait()
    for h in range(kv_heads):
        for w in range(2):
            st_rn[h, w, 0:fresh, :] = fresh_ref[:, w, columns_of(h)]
            for i in range(table):
                st_rn[h, w, fresh + i * page_rows:fresh + (i + 1) * page_rows, :] = pool_ref[table_ref[0, i], :, w, columns_of(h)]
    for k in range(1, share):
        start(st_rn.at[mine], kv_rn.at[share - k, 0], r_rn.at[share - k, 0], b, peer(k))
    for j in range(1, kv_heads):
        start(st_rn.at[flip(j)], kv_rn.at[0, j], r_rn.at[0, j], b, at_head(j))

    q_load.wait()
    for h in range(heads):
        q_turned[:, h * queries:(h + 1) * queries] = q_ref[:, h * HEAD_DIM:(h + 1) * HEAD_DIM].T

    scale = math.log2(math.e) / math.sqrt(HEAD_DIM)

    def attend(keys, values, bias, first):
        turned = values.T
        copies = BLOCK // bias.shape[1]
        wide = jnp.concatenate([bias] * copies, axis=1) if copies > 1 else bias
        for start_at in range(0, heads * queries, BLOCK):
            block = slice(start_at, start_at + BLOCK)
            s = jnp.dot(keys, q_turned[:, block], preferred_element_type=jnp.float32)
            s = s * scale + wide
            top = jnp.max(s, axis=0, keepdims=True)
            if not first:
                old = run_max[:, block]
                top = jnp.maximum(old, top)
            w = jnp.exp2(s - top)
            total = jnp.sum(w, axis=0, keepdims=True)
            high = w.astype(jnp.bfloat16)
            low = (w - high.astype(jnp.float32)).astype(jnp.bfloat16)
            out = jnp.dot(turned, high, preferred_element_type=jnp.float32)
            out = out + jnp.dot(turned, low, preferred_element_type=jnp.float32)
            if not first:
                shrink = jnp.exp2(old - top)
                total = total + run_sum[:, block] * shrink
                out = out + run_out[:, block] * shrink
            run_max[:, block] = top
            run_sum[:, block] = total
            run_out[:, block] = out

    def rows_of(kk, j):
        return st_rn.at[mine] if kk == 0 and j == 0 else kv_rn.at[kk, j]

    place = lax.broadcasted_iota(jnp.int32, (table * page_rows, LANES), 0)

    def attend_resident(spots, first=False):
        biases = []
        for kk, j in spots:
            live = shifted(metas[0, kk, j], bits * moves)
            biases.append(jnp.where(place < live, 0.0, NEG_LARGE))
        attend(
            jnp.concatenate([rows_of(kk, j)[0, fresh:] for kk, j in spots], axis=0),
            jnp.concatenate([rows_of(kk, j)[1, fresh:] for kk, j in spots], axis=0),
            jnp.concatenate(biases, axis=0), first,
        )

    def attend_fresh():
        spots = [(kk, j) for j in range(kv_heads) for kk in range(share)]
        line = lax.broadcasted_iota(jnp.int32, (fresh, queries), 0)
        column = lax.broadcasted_iota(jnp.int32, (fresh, queries), 1)
        biases = []
        for kk, j in spots:
            owner = flip(j) * share + lax.rem(member + kk, share)
            biases.append(jnp.where(line + owner * fresh <= column, 0.0, NEG_LARGE))
        attend(
            jnp.concatenate([rows_of(kk, j)[0, :fresh] for kk, j in spots], axis=0),
            jnp.concatenate([rows_of(kk, j)[1, :fresh] for kk, j in spots], axis=0),
            jnp.concatenate(biases, axis=0), False,
        )

    def attend_moved(spots):
        biases = []
        for i, kk, j in spots:
            chosen = picks(metas[1 + i, kk, j], b)
            for m in range(MOST):
                taken = chosen[m][0]
                for c in chosen[m][1:]:
                    taken = taken + c
                biases.append(jnp.broadcast_to(jnp.where(taken > 0, 0.0, NEG_LARGE), (page_rows, LANES)))
        attend(
            jnp.concatenate([kv_mov[i, kk, j, 0] for i, kk, j in spots], axis=0),
            jnp.concatenate([kv_mov[i, kk, j, 1] for i, kk, j in spots], axis=0),
            jnp.concatenate(biases, axis=0), False,
        )

    def relay_rows(j):
        arrived(kv_rn.at[0, j], r_rn.at[0, j])
        to_peers(kv_rn, r_rn, j)

    def peers_rows(j):
        for kk in range(1, share):
            arrived(kv_rn.at[kk, j], r_rn.at[kk, j])

    def relay_near(k, j):
        arrived(kv_mov.at[k, 0, j], r_mov.at[k, 0, j])
        to_peers(kv_mov, r_mov, k, j)

    def relay_far(e, j):
        i = near_count + e

        @pl.when(is_hub)
        def _():
            arrived(raw_far.at[e, j], r_far.at[e, j])
            row = metas[1 + i, 0, j]
            for k in range(1, half):
                select(raw_far.at[e, j], row, near(k), st_fwd.at[e, j, k - 1])
                start(st_fwd.at[e, j, k - 1], kv_mov.at[i, 0, j], r_mov.at[i, 0, j], near(k), a, hub_sent, (st_fwd, e, j, k - 1))
            select(raw_far.at[e, j], row, b, kv_mov.at[i, 0, j])

        if half > 1:
            @pl.when(jnp.logical_not(is_hub))
            def _():
                arrived(kv_mov.at[i, 0, j], r_mov.at[i, 0, j])

        to_peers(kv_mov, r_mov, i, j)

    def peers_moved(i, j):
        for kk in range(1, share):
            arrived(kv_mov.at[i, kk, j], r_mov.at[i, kk, j])

    def send_metas():
        for k in range(1, share):
            start(metas.at[0, 0], metas.at[0, share - k], r_meta.at[0, share - k], b, peer(k))
        start(metas.at[0, 0], metas.at[1 + near_count + reach, 0], r_meta.at[1 + near_count + reach, 0], far_hub, a)
        for k in range(1, half):
            start(metas.at[0, 0], metas.at[k, 0], r_meta.at[k, 0], near(k), a)

    def near_metas():
        for k in range(1, half):
            arrived(metas.at[k, 0], r_meta.at[k, 0])
            for p in range(1, share):
                start(metas.at[k, 0], metas.at[k, share - p], r_meta.at[k, share - p], b, peer(p))

    def far_metas(e):
        g = 1 + near_count + e
        arrived(metas.at[g, 0], r_meta.at[g, 0])
        if half > 1:
            @pl.when(is_hub)
            def _():
                for k in range(1, half):
                    start(metas.at[g, 0], metas.at[g, 0], r_meta.at[g, 0], near(k), a, hub_sent, (metas, g, 0))
        for p in range(1, share):
            start(metas.at[g, 0], metas.at[g, share - p], r_meta.at[g, share - p], b, peer(p))

    def peers_metas(g):
        for kk in range(1, share):
            arrived(metas.at[g, kk], r_meta.at[g, kk])

    members = range(share)
    for j in range(1, kv_heads):
        send_moved(j)
        if j == 1:
            attend_resident([(0, 0)], True)
    send_metas()
    for k in range(near_count):
        relay_near(k, 0)
    near_metas()
    for e in range(far_count):
        far_metas(e)
    for e in range(far_count):
        relay_far(e, 0)
    peers_metas(0)
    for j in range(1, kv_heads):
        peers_rows(0) if j == 1 else None
        if j == 1:
            attend_resident([(kk, 0) for kk in range(1, share)])
        relay_rows(j)
        for k in range(near_count):
            relay_near(k, j)
    for g in range(1, 1 + near_count + far_count):
        peers_metas(g)
    for j in range(1, kv_heads):
        for e in range(far_count):
            relay_far(e, j)
        peers_rows(j)
        attend_resident([(kk, j) for kk in members])
        for i in range(near_count):
            peers_moved(i, j - 1)
            attend_moved([(i, kk, j - 1) for kk in members])
        if j == kv_heads - 1:
            attend_fresh()
            for i in range(near_count):
                peers_moved(i, j)
                attend_moved([(i, kk, j) for kk in members])
        for e in range(far_count):
            peers_moved(near_count + e, j - 1)
        attend_moved([(near_count + e, kk, j - 1) for e in range(far_count) for kk in members])
    j = kv_heads - 1
    for e in range(far_count):
        peers_moved(near_count + e, j)
    attend_moved([(near_count + e, kk, j) for e in range(far_count) for kk in members])

    def turn(h):
        part = slice(h * queries, (h + 1) * queries)
        return (run_out[:, part] / run_sum[:, part]).T

    for h in range(heads):
        out_ref[:, h * HEAD_DIM:(h + 1) * HEAD_DIM] = turn(h).astype(out_ref.dtype)
    def left(src, n):
        remote(src, src, s_all.at[n], s_all.at[n], b, a).wait_send()

    for src, n in sent:
        left(src, n)
    if hub_sent:
        @pl.when(is_hub)
        def _():
            for spot, n in hub_sent:
                left(spot[0].at[spot[1:]], n)


def finish(append_ref, rows_ref, pool_ref, fresh_ref, out_ref, updated_ref):
    out_ref[...] = rows_ref[...]
    updated_ref[...] = pool_ref[...]
    updated_ref[append_ref[0, 0], 0:fresh_ref.shape[0]] = fresh_ref[...]


def local(n_inst, n_aa, queries, new_kv, pool, page_table, ctx_len, move_page, move_dest, append_page):
    pool_pages = pool[0]
    pages, page_rows, _, width = pool_pages.shape
    kv_heads = width // HEAD_DIM
    share = n_aa // kv_heads
    fresh_rows = new_kv[0]
    fresh_count = fresh_rows.shape[0]
    query_count, q_width = queries.shape[1:]
    heads = q_width // HEAD_DIM
    table = page_table.shape[1]
    moves = move_page.shape[1]
    half = n_inst // 2
    near, far = half - 1, half
    groups = 1 + near + far
    bf, f32 = jnp.bfloat16, jnp.float32
    dma = pltpu.SemaphoreType.DMA
    page = (2, page_rows, HEAD_DIM)
    slots = (2, MOST * page_rows, HEAD_DIM)
    rows = (2, fresh_count + table * page_rows, HEAD_DIM)
    attended = pl.pallas_call(
        functools.partial(kernel, n_inst, n_aa, kv_heads),
        out_shape=jax.ShapeDtypeStruct((query_count, q_width), bf),
        in_specs=[pl.BlockSpec(memory_space=pltpu.SMEM)] * 4 + [pl.BlockSpec(memory_space=pltpu.HBM)] * 3,
        out_specs=pl.BlockSpec(memory_space=pltpu.VMEM),
        scratch_shapes=[
            pltpu.VMEM((query_count, q_width), bf),
            pltpu.VMEM(pool_pages.shape, bf),
            pltpu.VMEM(fresh_rows.shape, bf),
            pltpu.VMEM((kv_heads, moves, *page), bf),
            pltpu.VMEM((kv_heads, *rows), bf),
            pltpu.VMEM((max(near, 1), kv_heads, *slots), bf),
            pltpu.VMEM((far, kv_heads, max(near, 1), *slots), bf),
            pltpu.VMEM((kv_heads, moves, *page), bf),
            pltpu.VMEM((far, kv_heads, moves, *page), bf),
            pltpu.VMEM((near + far, share, kv_heads, *slots), bf),
            pltpu.VMEM((share, kv_heads, *rows), bf),
            pltpu.VMEM((groups, share, kv_heads, 1, LANES), jnp.int32),
            pltpu.VMEM((1, heads * query_count), f32),
            pltpu.VMEM((1, heads * query_count), f32),
            pltpu.VMEM((HEAD_DIM, heads * query_count), f32),
            pltpu.VMEM((HEAD_DIM, heads * query_count), bf),
            dma((3,)), dma((400,)),
            dma((share, kv_heads)), dma((near + far, share, kv_heads)),
            dma((kv_heads,)), dma((far, kv_heads)), dma((kv_heads,)), dma((groups, share)),
        ],
        compiler_params=pltpu.CompilerParams(collective_id=0, has_side_effects=True, vmem_limit_bytes=48 * 2**20),
        name="paged_attention",
    )(page_table, ctx_len, move_page, move_dest, queries[0], pool_pages, fresh_rows)
    attended, updated = pl.pallas_call(
        finish,
        out_shape=(
            jax.ShapeDtypeStruct(attended.shape, bf),
            jax.ShapeDtypeStruct(pool_pages.shape, bf),
        ),
        in_specs=[pl.BlockSpec(memory_space=pltpu.SMEM)] + [pl.BlockSpec(memory_space=pltpu.VMEM)] * 3,
        out_specs=(pl.BlockSpec(memory_space=pltpu.VMEM),) * 2,
        compiler_params=pltpu.CompilerParams(vmem_limit_bytes=12 * 2**20),
        name="finish",
    )(append_page, attended, pool_pages, fresh_rows)
    return (attended[None], updated[None])


def solution(mesh):
    return jax.shard_map(
        functools.partial(local, mesh.shape["ba"], mesh.shape["aa"]),
        mesh=mesh,
        in_specs=(
            P("ba", None, "aa"),
            P("ba", "aa", None, None),
            P("ba", "aa", None, None, None),
            P("ba", "aa"),
            P("ba", "aa"),
            P("ba", "aa"),
            P("ba", "aa"),
            P("ba", "aa"),
        ),
        out_specs=(P("ba", None, "aa"), P("ba", "aa", None, None, None)),
        check_vma=False,
    )
```

```python
import functools
import math

import jax
import jax.numpy as jnp
from jax import lax
from jax.experimental import pallas as pl
from jax.experimental.pallas import tpu as pltpu
from jax.sharding import PartitionSpec as P

HEAD_DIM = 128
MOST = 2
LANES = 128
BLOCK = 256
NEG_LARGE = -1e30
MESH = pl.DeviceIdType.MESH


def kernel(
    n_inst, n_aa, kv_heads,
    table_ref, len_ref, page_ref, dest_ref, q_hbm, pool_hbm, fresh_hbm,
    out_ref,
    q_ref, pool_ref, fresh_ref,
    ext, st_rn, st_out, passed, kv_mov, kv_rn, metas,
    run_max, run_sum, run_out, q_turned,
    s_load, s_all, r_rn, r_mov, r_peer, r_pass, r_row, r_meta, s_wide,
):
    b = lax.axis_index("ba")
    a = lax.axis_index("aa")
    share = n_aa // kv_heads
    mine, member = a // share, a % share
    half = n_inst // 2
    side = b // half
    base = side * half
    pos = b - base
    hub = half - 1 + side
    far_hub = half - side
    is_hub = b == hub
    reach = (1 - side) * (half - 1 - pos) + side * pos
    near_count = half - 1
    table = table_ref.shape[1]
    moves = page_ref.shape[1]
    page_rows = pool_ref.shape[1]
    fresh = fresh_ref.shape[0]
    queries = q_ref.shape[0]
    heads = q_ref.shape[1] // HEAD_DIM
    bits = (n_inst - 1).bit_length()
    shared = half == 2 and MOST == 2 and moves < 2 * MOST

    def near(k):
        return base + lax.rem(pos + k + half, half)

    def far(t):
        return far_hub + (1 - 2 * side) * t

    def flip(j):
        to = mine
        bit = 1
        while bit <= j:
            if j & bit:
                to = to + bit - 2 * bit * (mine // bit % 2)
            bit *= 2
        return to

    heads_at = [flip(j) for j in range(kv_heads)]
    device_at = [h * share + member for h in heads_at]
    peers = [mine * share + lax.rem(member + k, share) for k in range(share)]

    pool_load = pltpu.make_async_copy(pool_hbm, pool_ref, s_load.at[0])
    pool_load.start()
    q_load = pltpu.make_async_copy(q_hbm, q_ref, s_load.at[1])
    fresh_load = pltpu.make_async_copy(fresh_hbm, fresh_ref, s_load.at[2])
    fresh_load.start()
    q_load.start()

    barrier = pltpu.get_barrier_semaphore()
    partners = [(b, device_at[j]) for j in range(1, kv_heads)]
    partners += [(b, peers[k]) for k in range(1, share)]
    partners += [(near(k), to) for k in range(1, half) for to in device_at]
    partners += [(far(t), a) for t in range(half)]
    for ba, aa in partners:
        pl.semaphore_signal(barrier, inc=1, device_id={"ba": ba, "aa": aa}, device_id_type=MESH)

    def columns_of(h):
        return slice(h * HEAD_DIM, (h + 1) * HEAD_DIM)

    code = len_ref[0, 0]
    for i in range(moves):
        code = code * (1 << bits) + dest_ref[0, i]
    metas[0, 0, 0] = jnp.full((1, LANES), code, jnp.int32)

    def chosen_for(target):
        seen = jnp.int32(0)
        picked = [jnp.int32(0) for _ in range(MOST)]
        for i in range(moves):
            hit = (dest_ref[0, i] == target).astype(jnp.int32)
            for m in range(MOST):
                picked[m] = picked[m] + hit * (seen == m).astype(jnp.int32) * i
            seen = seen + hit
        return picked, seen

    outs = [(0, t, m) for m in reversed(range(1, MOST)) for t in range(half) if not (shared and t)]
    first_cut = len(outs)
    outs += [(0, t, 0) for t in reversed(range(half))]
    second_cut = len(outs)
    outs += [(1, k, m) for k in range(1, half) for m in range(MOST)]
    cuts = [(0, first_cut), (first_cut, second_cut)]
    out_count = st_out.shape[0] // kv_heads

    pool_load.wait()
    for i in range(moves):
        for h in range(kv_heads):
            for w in range(2):
                ext[i, h, w] = pool_ref[page_ref[0, i], :, w, columns_of(h)]
    picked_far = [chosen_for(far(t)) for t in range(half)]
    picked_near = [chosen_for(near(k)) for k in range(half)]
    for n, (kind, t, m) in enumerate(outs):
        index = (picked_near if kind else picked_far)[t][0][m]
        if shared and not kind and m == 1:
            index = jnp.where(picked_far[0][1] > 1, index, picked_far[1][0][1])
        for h in range(kv_heads):
            st_out[h * out_count + n] = ext[index, h]

    def remote(src, dst, ss, rs, ba, aa):
        return pltpu.make_async_remote_copy(
            src_ref=src, dst_ref=dst, send_sem=ss, recv_sem=rs,
            device_id={"ba": ba, "aa": aa}, device_id_type=MESH,
        )

    groups = metas.shape[0]
    wide = []
    pages = st_out.shape[0]
    kinds = {
        "page": (pages, lambda r: st_out.at[0:r]),
        "hub": (pages, lambda r: st_out.at[0:r]),
        "leaf": (pages, lambda r: st_out.at[0:r]),
        "pair": (pages // MOST, lambda r: st_out.at[0:r * MOST]),
        "rows": (kv_heads, lambda r: st_rn.at[0:r]),
        "row": (kv_heads, lambda r: metas.at[0, 0, 0:r]),
        "block": (groups, lambda r: metas.at[0:r, 0]),
    }
    names = list(kinds)
    counts = {name: 0 for name in names}
    per_kind = s_all.shape[1]

    def start(kind, src, dst, rs, ba, aa):
        n = counts[kind] // kinds[kind][0]
        assert n < per_kind
        counts[kind] += 1
        remote(src, dst, s_all.at[names.index(kind), n], rs, ba, aa).start()

    def all_left(kind):
        size, piece = kinds[kind]
        for n in range(0, counts[kind], size):
            ref = piece(min(size, counts[kind] - n))
            remote(ref, ref, s_all.at[names.index(kind), n // size], s_load.at[0], b, a).wait_send()

    def arrived(slot, rs):
        remote(slot, slot, s_load.at[0], rs, b, a).wait_recv()

    def shifted(row, count):
        return lax.shift_right_logical(row, jnp.full(row.shape, count, jnp.int32))

    def taken(row, target):
        low = jnp.full(row.shape, (1 << bits) - 1, jnp.int32)
        count = jnp.zeros(row.shape, jnp.int32)
        for i in range(moves):
            dest = lax.bitwise_and(shifted(row, bits * (moves - 1 - i)), low)
            count = count + (dest == target).astype(jnp.int32)
        return count

    fresh_load.wait()
    for h in range(kv_heads):
        for w in range(2):
            st_rn[h, w, 0:fresh, :] = fresh_ref[:, w, columns_of(h)]
            for i in range(table):
                st_rn[h, w, fresh + i * page_rows:fresh + (i + 1) * page_rows, :] = pool_ref[table_ref[0, i], :, w, columns_of(h)]
    pl.semaphore_wait(barrier, len(partners))

    def source(j, lo, hi):
        return st_out.at[pl.ds(mine * out_count + lo, hi - lo)] if j == 0 else passed.at[j, lo:hi]

    def send_on(j, part):
        lo, hi = cuts[part]
        if j:
            arrived(passed.at[j, lo:hi], r_pass.at[j, part])
        i = near_count + reach
        for n in range(lo, hi):
            _, t, m = outs[n]
            start("page", source(j, n, n + 1), kv_mov.at[i, 0, j, m:m + 1], r_mov.at[i, j, m], far(t), a)

    def send_near(j):
        for k in range(1, half):
            n = second_cut + (k - 1) * MOST
            start("pair", st_out.at[pl.ds(heads_at[j] * out_count + n, MOST)], kv_mov.at[k - 1, 0, j], r_mov.at[k - 1, j, 0], near(k), device_at[j])

    def send_plane(j, part):
        lo, hi = cuts[part]
        kind = {1: "page", 2: "pair"}
        src, dst = st_out.at[pl.ds(heads_at[j] * out_count + lo, hi - lo)], passed.at[j, lo:hi]
        if hi - lo in kind:
            start(kind[hi - lo], src, dst, r_pass.at[j, part], b, device_at[j])
        else:
            wide.append((src, j, part))
            remote(src, dst, s_wide.at[j, part], r_pass.at[j, part], b, device_at[j]).start()

    send_on(0, 0)
    for j in range(1, kv_heads):
        start("row", metas.at[0, 0, 0], metas.at[0, 0, j], r_row.at[0], b, device_at[j])
    for j in range(1, kv_heads):
        send_plane(j, 0)
    send_near(0)
    send_on(0, 1)
    for j in range(1, kv_heads):
        send_plane(j, 1)
    for k in range(1, share):
        start("rows", st_rn.at[mine], kv_rn.at[share - k, 0], r_rn.at[share - k, 0], b, peers[k])

    q_load.wait()
    for h in range(heads):
        q_turned[:, h * queries:(h + 1) * queries] = q_ref[:, h * HEAD_DIM:(h + 1) * HEAD_DIM].T

    scale = math.log2(math.e) / math.sqrt(HEAD_DIM)

    def attend(keys, values, bias, first):
        turned = values.T
        copies = BLOCK // bias.shape[1]
        wide = jnp.concatenate([bias] * copies, axis=1) if copies > 1 else bias
        for start_at in range(0, heads * queries, BLOCK):
            block = slice(start_at, start_at + BLOCK)
            s = jnp.dot(keys, q_turned[:, block], preferred_element_type=jnp.float32)
            s = s * scale + wide
            top = jnp.max(s, axis=0, keepdims=True)
            if not first:
                old = run_max[:, block]
                top = jnp.maximum(old, top)
            w = jnp.exp2(s - top)
            total = jnp.sum(w, axis=0, keepdims=True)
            high = w.astype(jnp.bfloat16)
            low = (w - high.astype(jnp.float32)).astype(jnp.bfloat16)
            out = jnp.dot(turned, high, preferred_element_type=jnp.float32)
            out = out + jnp.dot(turned, low, preferred_element_type=jnp.float32)
            if not first:
                shrink = jnp.exp2(old - top)
                total = total + run_sum[:, block] * shrink
                out = out + run_out[:, block] * shrink
            run_max[:, block] = top
            run_sum[:, block] = total
            run_out[:, block] = out

    def rows_of(kk, j):
        return st_rn.at[mine] if kk == 0 and j == 0 else kv_rn.at[kk, j]

    place = lax.broadcasted_iota(jnp.int32, (table * page_rows, LANES), 0)

    def attend_resident(spots, first=False):
        biases = []
        for kk, j in spots:
            live = shifted(metas[0, kk, j], bits * moves)
            biases.append(jnp.where(place < live, 0.0, NEG_LARGE))
        attend(
            jnp.concatenate([rows_of(kk, j)[0, fresh:] for kk, j in spots], axis=0),
            jnp.concatenate([rows_of(kk, j)[1, fresh:] for kk, j in spots], axis=0),
            jnp.concatenate(biases, axis=0), first,
        )

    def attend_fresh():
        spots = [(kk, j) for j in range(kv_heads) for kk in range(share)]
        line = lax.broadcasted_iota(jnp.int32, (fresh, queries), 0)
        column = lax.broadcasted_iota(jnp.int32, (fresh, queries), 1)
        biases = []
        for kk, j in spots:
            owner = heads_at[j] * share + lax.rem(member + kk, share)
            biases.append(jnp.where(line + owner * fresh <= column, 0.0, NEG_LARGE))
        attend(
            jnp.concatenate([rows_of(kk, j)[0, :fresh] for kk, j in spots], axis=0),
            jnp.concatenate([rows_of(kk, j)[1, :fresh] for kk, j in spots], axis=0),
            jnp.concatenate(biases, axis=0), False,
        )

    def attend_moved(spots):
        biases = []
        for i, kk, j, m in spots:
            count = taken(metas[1 + i, kk, j], b)
            biases.append(jnp.broadcast_to(jnp.where(count > m, 0.0, NEG_LARGE), (page_rows, LANES)))
        attend(
            jnp.concatenate([kv_mov[i, kk, j, m, 0] for i, kk, j, m in spots], axis=0),
            jnp.concatenate([kv_mov[i, kk, j, m, 1] for i, kk, j, m in spots], axis=0),
            jnp.concatenate(biases, axis=0), False,
        )

    members = range(share)
    chips = range(kv_heads)
    slots = range(MOST)

    def relay_rows(j):
        arrived(kv_rn.at[0, j], r_rn.at[0, j])
        for k in range(1, share):
            start("rows", kv_rn.at[0, j], kv_rn.at[share - k, j], r_rn.at[share - k, j], b, peers[k])

    def peers_rows(j):
        for kk in range(1, share):
            arrived(kv_rn.at[kk, j], r_rn.at[kk, j])

    def relay_near(j):
        for k in range(near_count):
            arrived(kv_mov.at[k, 0, j], r_mov.at[k, j, 0])
            for p in range(1, share):
                start("pair", kv_mov.at[k, 0, j], kv_mov.at[k, share - p, j], r_peer.at[k, share - p - 1, j // 2], b, peers[p])

    def relay_far(e, j, m):
        i = near_count + e
        spot = kv_mov.at[i, 0, j, m]
        arrived(spot, r_mov.at[i, j, m])
        for p in range(1, share):
            start("page", spot, kv_mov.at[i, share - p, j, m], r_peer.at[i, share - p - 1, m], b, peers[p])

    def hub_relay(spots):
        @pl.when(is_hub)
        def _():
            for e, j in spots:
                i = near_count + e
                spot = kv_mov.at[i, 0, j, 1]
                arrived(spot, r_mov.at[i, j, 1])
                start("hub", spot, kv_mov.at[i, 0, j, 1], r_mov.at[i, j, 1], near(1), a)
                for p in range(1, share):
                    start("hub", spot, kv_mov.at[i, share - p, j, 1], r_peer.at[i, share - p - 1, 1], b, peers[p])

    def leaf_relay(spots):
        @pl.when(jnp.logical_not(is_hub))
        def _():
            for e, j in spots:
                i = near_count + e
                spot = kv_mov.at[i, 0, j, 1]
                arrived(spot, r_mov.at[i, j, 1])
                for p in range(1, share):
                    start("leaf", spot, kv_mov.at[i, share - p, j, 1], r_peer.at[i, share - p - 1, 1], b, peers[p])

    def send_metas():
        arrived(metas.at[0, 0, 1:kv_heads], r_row.at[0])
        block = metas.at[0, 0]
        for t in range(half):
            g = 1 + near_count + reach
            start("block", block, metas.at[g, 0], r_meta.at[g, 0], far(t), a)
        for k in range(1, half):
            start("block", block, metas.at[k, 0], r_meta.at[k, 0], near(k), a)
        for p in range(1, share):
            start("block", block, metas.at[0, share - p], r_meta.at[0, share - p], b, peers[p])

    def relay_metas():
        for g in range(1, groups):
            arrived(metas.at[g, 0], r_meta.at[g, 0])
            for p in range(1, share):
                start("block", metas.at[g, 0], metas.at[g, share - p], r_meta.at[1, share - p], b, peers[p])

    def peers_metas(lo, hi):
        for kk in range(1, share):
            arrived(metas.at[lo:hi, kk], r_meta.at[lo, kk])

    def do_resident(j):
        peers_rows(j)
        attend_resident([(kk, j) for kk in members])

    def do_near(part):
        js = list(chips)[2 * part:2 * part + 2]
        for k in range(near_count):
            for kk in range(1, share):
                arrived(kv_mov.at[k, kk, js[0]:js[-1] + 1], r_peer.at[k, kk - 1, part])
            attend_moved([(k, kk, j, m) for j in js for kk in members for m in slots])

    def do_far(e, m):
        i = near_count + e
        for kk in range(1, share):
            arrived(kv_mov.at[i, kk, :, m], r_peer.at[i, kk - 1, m])
        attend_moved([(i, kk, j, m) for j in chips for kk in members])

    late = [m for m in reversed(slots) if m == 0 or not shared]

    def relay_late(j):
        for e in range(half):
            for m in late:
                relay_far(e, j, m)

    attend_resident([(0, 0)], True)
    send_on(1, 0)
    send_on(2, 0)
    send_metas()
    peers_metas(0, 1)
    send_on(3, 0)
    send_on(1, 1)
    send_on(2, 1)
    for j in range(1, kv_heads):
        send_near(j)
    peers_rows(0)
    attend_resident([(kk, 0) for kk in range(1, share)])
    if shared:
        hub_relay([(0, 0), (1, 0), (0, 1)])
    send_on(3, 1)
    for j in range(1, kv_heads):
        start("rows", st_rn.at[heads_at[j]], kv_rn.at[0, j], r_rn.at[0, j], b, device_at[j])
    relay_metas()
    if shared:
        hub_relay([(0, 2), (0, 3), (1, 1)])
    relay_near(0)
    relay_late(0)
    if shared:
        hub_relay([(1, 2), (1, 3)])
    relay_near(1)
    peers_metas(1, groups)
    do_near(0)
    relay_rows(1)
    relay_rows(2)
    relay_near(2)
    relay_late(1)
    do_resident(1)
    relay_rows(3)
    relay_near(3)
    do_resident(2)
    relay_late(2)
    do_near(1)
    do_resident(3)
    relay_late(3)
    attend_fresh()
    if shared:
        leaf_relay([(e, j) for j in chips for e in range(half)])
        do_far(0, 1)
        do_far(1, 1)
    for m in late:
        for e in range(half):
            do_far(e, m)

    def turn(h):
        part = slice(h * queries, (h + 1) * queries)
        return (run_out[:, part] / run_sum[:, part]).T

    for h in range(heads):
        out_ref[:, h * HEAD_DIM:(h + 1) * HEAD_DIM] = turn(h).astype(out_ref.dtype)

    for name in names:
        if name not in ("hub", "leaf"):
            all_left(name)
    for src, j, part in wide:
        remote(src, src, s_wide.at[j, part], s_load.at[0], b, a).wait_send()
    if shared:
        @pl.when(is_hub)
        def _():
            all_left("hub")

        @pl.when(jnp.logical_not(is_hub))
        def _():
            all_left("leaf")


def finish(append_ref, rows_ref, pool_ref, fresh_ref, out_ref, updated_ref):
    out_ref[...] = rows_ref[...]
    updated_ref[...] = pool_ref[...]
    updated_ref[append_ref[0, 0], 0:fresh_ref.shape[0]] = fresh_ref[...]


def local(n_inst, n_aa, queries, new_kv, pool, page_table, ctx_len, move_page, move_dest, append_page):
    pool_pages = pool[0]
    pages, page_rows, _, width = pool_pages.shape
    kv_heads = width // HEAD_DIM
    share = n_aa // kv_heads
    fresh_rows = new_kv[0]
    fresh_count = fresh_rows.shape[0]
    query_count, q_width = queries.shape[1:]
    heads = q_width // HEAD_DIM
    table = page_table.shape[1]
    moves = move_page.shape[1]
    half = n_inst // 2
    near = half - 1
    groups = 1 + near + half
    out_count = (near + half) * MOST
    per_kind = 3 if share < 4 else 9
    bf, f32 = jnp.bfloat16, jnp.float32
    dma = pltpu.SemaphoreType.DMA
    page = (2, page_rows, HEAD_DIM)
    rows = (2, fresh_count + table * page_rows, HEAD_DIM)
    attended = pl.pallas_call(
        functools.partial(kernel, n_inst, n_aa, kv_heads),
        out_shape=pltpu.VMEM((query_count, q_width), bf),
        in_specs=[pl.BlockSpec(memory_space=pltpu.SMEM)] * 4 + [pl.BlockSpec(memory_space=pltpu.HBM)] * 3,
        out_specs=pl.BlockSpec(memory_space=pltpu.VMEM),
        scratch_shapes=[
            pltpu.VMEM((query_count, q_width), bf),
            pltpu.VMEM(pool_pages.shape, bf),
            pltpu.VMEM(fresh_rows.shape, bf),
            pltpu.VMEM((moves, kv_heads, *page), bf),
            pltpu.VMEM((kv_heads, *rows), bf),
            pltpu.VMEM((kv_heads * out_count, *page), bf),
            pltpu.VMEM((kv_heads, out_count, *page), bf),
            pltpu.VMEM((near + half, share, kv_heads, MOST, *page), bf),
            pltpu.VMEM((share, kv_heads, *rows), bf),
            pltpu.VMEM((groups, share, kv_heads, 1, LANES), jnp.int32),
            pltpu.VMEM((1, heads * query_count), f32),
            pltpu.VMEM((1, heads * query_count), f32),
            pltpu.VMEM((HEAD_DIM, heads * query_count), f32),
            pltpu.VMEM((HEAD_DIM, heads * query_count), bf),
            dma((3,)), dma((7, per_kind)),
            dma((share, kv_heads)), dma((near + half, kv_heads, MOST)), dma((near + half, share - 1, MOST)),
            dma((kv_heads, 2)), dma((1,)), dma((groups, share)), dma((kv_heads, 2) if half > 2 else (1, 1)),
        ],
        compiler_params=pltpu.CompilerParams(collective_id=0, has_side_effects=True, vmem_limit_bytes=60 * 2**20),
        name="paged_attention",
    )(page_table, ctx_len, move_page, move_dest, queries[0], pool_pages, fresh_rows)
    attended, updated = pl.pallas_call(
        finish,
        out_shape=(
            jax.ShapeDtypeStruct(attended.shape, bf),
            jax.ShapeDtypeStruct(pool_pages.shape, bf),
        ),
        in_specs=[pl.BlockSpec(memory_space=pltpu.SMEM)] + [pl.BlockSpec(memory_space=pltpu.VMEM)] * 3,
        out_specs=(pl.BlockSpec(memory_space=pltpu.VMEM),) * 2,
        compiler_params=pltpu.CompilerParams(vmem_limit_bytes=12 * 2**20),
        name="finish",
    )(append_page, attended, pool_pages, fresh_rows)
    return (attended[None], updated[None])


def solution(mesh):
    return jax.shard_map(
        functools.partial(local, mesh.shape["ba"], mesh.shape["aa"]),
        mesh=mesh,
        in_specs=(
            P("ba", None, "aa"),
            P("ba", "aa", None, None),
            P("ba", "aa", None, None, None),
            P("ba", "aa"),
            P("ba", "aa"),
            P("ba", "aa"),
            P("ba", "aa"),
            P("ba", "aa"),
        ),
        out_specs=(P("ba", None, "aa"), P("ba", "aa", None, None, None)),
        check_vma=False,
    )
```

```python
import functools
import math

import jax
import jax.numpy as jnp
from jax import lax
from jax.experimental import pallas as pl
from jax.experimental.pallas import tpu as pltpu
from jax.sharding import PartitionSpec as P

HEAD_DIM = 128
MOST = 2
LANES = 128
BLOCK = 256
NEG_LARGE = -1e30
MESH = pl.DeviceIdType.MESH


def kernel(
    n_inst, n_aa, kv_heads,
    table_hbm, len_hbm, page_hbm, dest_hbm, q_hbm, pool_hbm, fresh_hbm,
    out_ref,
    table_ref, len_ref, page_ref, dest_ref, q_ref, pool_ref, fresh_ref,
    ext, st_rn, st_out, passed, kv_mov, kv_rn, metas,
    run_max, run_sum, spare_score, run_out, q_turned,
    s_load, s_all, r_rn, r_mov, r_peer, r_pass, r_meta, s_wide,
):
    b = lax.axis_index("ba")
    a = lax.axis_index("aa")
    share = n_aa // kv_heads
    mine, member = a // share, a % share
    half = n_inst // 2
    side = b // half
    base = side * half
    pos = b - base
    hub = half - 1 + side
    far_hub = half - side
    is_hub = b == hub
    reach = (1 - side) * (half - 1 - pos) + side * pos
    near_count = half - 1
    table = table_ref.shape[1]
    moves = page_ref.shape[1]
    page_rows = pool_ref.shape[1]
    fresh = fresh_ref.shape[0]
    queries = q_ref.shape[0]
    heads = q_ref.shape[1] // HEAD_DIM
    bits = (n_inst - 1).bit_length()
    shared = half == 2 and MOST == 2 and moves < 2 * MOST

    def near(k):
        return base + lax.rem(pos + k + half, half)

    def far(t):
        return far_hub + (1 - 2 * side) * t

    def flip(j):
        to = mine
        bit = 1
        while bit <= j:
            if j & bit:
                to = to + bit - 2 * bit * (mine // bit % 2)
            bit *= 2
        return to

    heads_at = [flip(j) for j in range(kv_heads)]
    device_at = [h * share + member for h in heads_at]
    peers = [mine * share + lax.rem(member + k, share) for k in range(share)]

    pool_load = pltpu.make_async_copy(pool_hbm, pool_ref, s_load.at[0])
    pool_load.start()
    q_load = pltpu.make_async_copy(q_hbm, q_ref, s_load.at[1])
    fresh_load = pltpu.make_async_copy(fresh_hbm, fresh_ref, s_load.at[2])
    small = []
    for n, (src, dst) in enumerate(((page_hbm, page_ref), (dest_hbm, dest_ref), (len_hbm, len_ref), (table_hbm, table_ref))):
        small.append(pltpu.make_async_copy(src, dst, s_load.at[3 + n]))
        small[-1].start()
    fresh_load.start()
    q_load.start()

    barrier = pltpu.get_barrier_semaphore()
    partners = [
        (b, heads_at[j] * share + lax.rem(member + k, share))
        for j in range(kv_heads) for k in range(share) if j or k
    ]
    partners += [(near(k), to) for k in range(1, half) for to in device_at]
    partners += [(far(t), a) for t in range(half)]
    for ba, aa in partners:
        pl.semaphore_signal(barrier, inc=1, device_id={"ba": ba, "aa": aa}, device_id_type=MESH)

    def columns_of(h):
        return slice(h * HEAD_DIM, (h + 1) * HEAD_DIM)

    for load in small:
        load.wait()
    code = len_ref[0, 0]
    for i in range(moves):
        code = code * (1 << bits) + dest_ref[0, i]
    metas[0, 0, 0] = jnp.full((1, LANES), code, jnp.int32)

    def chosen_for(target):
        seen = jnp.int32(0)
        picked = [jnp.int32(0) for _ in range(MOST)]
        for i in range(moves):
            hit = (dest_ref[0, i] == target).astype(jnp.int32)
            for m in range(MOST):
                picked[m] = picked[m] + hit * (seen == m).astype(jnp.int32) * i
            seen = seen + hit
        return picked, seen

    outs = [(0, t, m) for m in reversed(range(1, MOST)) for t in range(half) if not (shared and t)]
    first_cut = len(outs)
    outs += [(0, t, 0) for t in reversed(range(half))]
    second_cut = len(outs)
    outs += [(1, k, m) for k in range(1, half) for m in range(MOST)]
    cuts = [(0, first_cut), (first_cut, second_cut)]
    out_count = st_out.shape[0] // kv_heads

    pool_load.wait()
    for i in range(moves):
        turned = jnp.swapaxes(pool_ref[page_ref[0, i]], 0, 1)
        for h in range(kv_heads):
            ext[i, h] = turned[:, :, columns_of(h)]
    picked_far = [chosen_for(far(t)) for t in range(half)]
    picked_near = [chosen_for(near(k)) for k in range(half)]
    for n, (kind, t, m) in enumerate(outs):
        index = (picked_near if kind else picked_far)[t][0][m]
        if shared and not kind and m == 1:
            index = jnp.where(picked_far[0][1] > 1, index, picked_far[1][0][1])
        for h in range(kv_heads):
            st_out[h * out_count + n] = ext[index, h]

    def remote(src, dst, ss, rs, ba, aa):
        return pltpu.make_async_remote_copy(
            src_ref=src, dst_ref=dst, send_sem=ss, recv_sem=rs,
            device_id={"ba": ba, "aa": aa}, device_id_type=MESH,
        )

    groups = metas.shape[0]
    wide = []
    pages = st_out.shape[0]
    kinds = {
        "page": (pages, lambda r: st_out.at[0:r]),
        "hub": (pages, lambda r: st_out.at[0:r]),
        "leaf": (pages, lambda r: st_out.at[0:r]),
        "pair": (pages // MOST, lambda r: st_out.at[0:r * MOST]),
        "rows": (kv_heads, lambda r: st_rn.at[0:r]),
        "row": (kv_heads, lambda r: metas.at[0, 0, 0:r]),
        "block": (groups, lambda r: metas.at[0:r, 0]),
    }
    names = list(kinds)
    counts = {name: 0 for name in names}
    per_kind = s_all.shape[1]

    def start(kind, src, dst, rs, ba, aa):
        n = counts[kind] // kinds[kind][0]
        assert n < per_kind
        counts[kind] += 1
        remote(src, dst, s_all.at[names.index(kind), n], rs, ba, aa).start()

    def all_left(kind):
        size, piece = kinds[kind]
        for n in range(0, counts[kind], size):
            ref = piece(min(size, counts[kind] - n))
            remote(ref, ref, s_all.at[names.index(kind), n // size], s_load.at[0], b, a).wait_send()

    def arrived(slot, rs):
        remote(slot, slot, s_load.at[0], rs, b, a).wait_recv()

    def shifted(row, count):
        return lax.shift_right_logical(row, jnp.full(row.shape, count, jnp.int32))

    def taken(row, target):
        low = jnp.full(row.shape, (1 << bits) - 1, jnp.int32)
        count = jnp.zeros(row.shape, jnp.int32)
        for i in range(moves):
            dest = lax.bitwise_and(shifted(row, bits * (moves - 1 - i)), low)
            count = count + (dest == target).astype(jnp.int32)
        return count

    fresh_load.wait()
    for lo, block in [(0, 0)] + [(fresh + i * page_rows, i) for i in range(table)]:
        turned = jnp.swapaxes(fresh_ref[...] if lo == 0 else pool_ref[table_ref[0, block]], 0, 1)
        for h in range(kv_heads):
            st_rn[h, :, lo:lo + turned.shape[1], :] = turned[:, :, columns_of(h)]
    pl.semaphore_wait(barrier, len(partners))

    def source(j, lo, hi):
        return st_out.at[pl.ds(mine * out_count + lo, hi - lo)] if j == 0 else passed.at[j, lo:hi]

    def send_on(j, part):
        lo, hi = cuts[part]
        if j:
            arrived(passed.at[j, lo:hi], r_pass.at[j, part])
        i = near_count + reach
        for n in range(lo, hi):
            _, t, m = outs[n]
            start("page", source(j, n, n + 1), kv_mov.at[i, 0, j, m:m + 1], r_mov.at[i, j, m], far(t), a)

    def send_near(j):
        for k in range(1, half):
            n = second_cut + (k - 1) * MOST
            start("pair", st_out.at[pl.ds(heads_at[j] * out_count + n, MOST)], kv_mov.at[k - 1, 0, j], r_mov.at[k - 1, j, 0], near(k), device_at[j])

    def send_plane(j, part):
        lo, hi = cuts[part]
        kind = {1: "page", 2: "pair"}
        src, dst = st_out.at[pl.ds(heads_at[j] * out_count + lo, hi - lo)], passed.at[j, lo:hi]
        if hi - lo in kind:
            start(kind[hi - lo], src, dst, r_pass.at[j, part], b, device_at[j])
        else:
            wide.append((src, j, part))
            remote(src, dst, s_wide.at[j, part], r_pass.at[j, part], b, device_at[j]).start()

    send_on(0, 0)
    for j in range(1, kv_heads):
        send_plane(j, 0)
    send_on(0, 1)
    for j in range(kv_heads):
        for k in range(share):
            if j or k:
                to = heads_at[j] * share + lax.rem(member + k, share)
                kk = (share - k) % share
                start("row", metas.at[0, 0, 0], metas.at[0, kk, j], r_meta.at[0, kk], b, to)
    for j in range(kv_heads):
        send_near(j)
    for j in range(1, kv_heads):
        send_plane(j, 1)
    for k in range(1, share):
        start("rows", st_rn.at[mine], kv_rn.at[share - k, 0], r_rn.at[share - k, 0], b, peers[k])
    for j in range(1, kv_heads):
        start("rows", st_rn.at[heads_at[j]], kv_rn.at[0, j], r_rn.at[0, j], b, device_at[j])

    q_load.wait()
    scale = math.log2(math.e) / math.sqrt(HEAD_DIM)
    for h in range(heads):
        part = slice(h * queries, (h + 1) * queries)
        turned = q_ref[:, h * HEAD_DIM:(h + 1) * HEAD_DIM].T.astype(jnp.float32) * scale
        high = turned.astype(jnp.bfloat16)
        q_turned[0:HEAD_DIM, part] = high
        q_turned[HEAD_DIM:2 * HEAD_DIM, part] = (turned - high.astype(jnp.float32)).astype(jnp.bfloat16)

    def attend(keys, values, keep, hidden, bias, first):
        left = values.T
        if bias is None:
            left = left * keep
            hidden = jnp.concatenate([hidden] * (BLOCK // LANES), axis=1)
        else:
            bias = jnp.concatenate([bias] * (BLOCK // bias.shape[1]), axis=1)
        both = jnp.concatenate([keys, keys], axis=1)
        for start_at in range(0, heads * queries, BLOCK):
            block = slice(start_at, start_at + BLOCK)
            s = jnp.dot(both, q_turned[:, block], preferred_element_type=jnp.float32)
            if bias is not None:
                s = s + bias
            top = jnp.max(s, axis=0, keepdims=True)
            if not first:
                old = run_max[:, block]
                top = jnp.maximum(old, top)
            w = jnp.exp2(s - top)
            total = jnp.sum(w, axis=0, keepdims=True)
            if bias is None:
                total = total - hidden * jnp.exp2(spare_score[:, block] - top)
            high = w.astype(jnp.bfloat16)
            low = (w - high.astype(jnp.float32)).astype(jnp.bfloat16)
            out = jnp.dot(left, high, preferred_element_type=jnp.float32)
            out = out + jnp.dot(left, low, preferred_element_type=jnp.float32)
            if not first:
                shrink = jnp.exp2(old - top)
                total = total + run_sum[:, block] * shrink
                out = out + run_out[:, block] * shrink
            run_max[:, block] = top
            run_sum[:, block] = total
            run_out[:, block] = out

    def rows_of(kk, j):
        return st_rn.at[mine] if kk == 0 and j == 0 else kv_rn.at[kk, j]

    chunk = table * page_rows
    place = lax.broadcasted_iota(jnp.int32, (chunk, LANES), 0)
    lane = lax.broadcasted_iota(jnp.int32, (1, chunk), 1)
    slot_lane = lax.broadcasted_iota(jnp.int32, (1, LANES), 1)
    spare = st_rn[mine, 0, fresh:fresh + 16, :]
    for start_at in range(0, heads * queries, BLOCK):
        block = slice(start_at, start_at + BLOCK)
        spare_score[:, block] = jnp.dot(
            jnp.concatenate([spare, spare], axis=1), q_turned[:, block], preferred_element_type=jnp.float32
        )[0:1]
    spare = spare[0:1].astype(jnp.float32)

    def visible(mask, keys):
        return jnp.where(mask, keys.astype(jnp.float32), spare).astype(jnp.bfloat16)

    def attend_resident(spots, first=False):
        keys, values, keep = [], [], []
        hidden = jnp.zeros((1, LANES), jnp.int32)
        for kk, j in spots:
            live = shifted(metas[0, kk, j], bits * moves)
            rows = rows_of(kk, j)
            keys.append(visible(place < live, rows[0, fresh:]))
            values.append(rows[1, fresh:])
            wide_live = jnp.concatenate([live] * (chunk // LANES), axis=1)
            keep.append(jnp.where(lane < wide_live, 1.0, 0.0))
            hidden = hidden + (chunk - live)
        attend(
            jnp.concatenate(keys, axis=0), jnp.concatenate(values, axis=0),
            jnp.concatenate(keep, axis=1).astype(jnp.bfloat16), hidden.astype(jnp.float32), None, first,
        )

    def attend_fresh():
        spots = [(kk, j) for j in range(kv_heads) for kk in range(share)]
        line = lax.broadcasted_iota(jnp.int32, (fresh, queries), 0)
        column = lax.broadcasted_iota(jnp.int32, (fresh, queries), 1)
        biases = []
        for kk, j in spots:
            owner = heads_at[j] * share + lax.rem(member + kk, share)
            biases.append(jnp.where(line + owner * fresh <= column, 0.0, NEG_LARGE))
        attend(
            jnp.concatenate([rows_of(kk, j)[0, :fresh] for kk, j in spots], axis=0),
            jnp.concatenate([rows_of(kk, j)[1, :fresh] for kk, j in spots], axis=0),
            None, None, jnp.concatenate(biases, axis=0), False,
        )

    def attend_moved(spots):
        along = LANES // page_rows
        keys, keep = [], []
        hidden = jnp.zeros((1, LANES), jnp.float32)
        for n, (i, kk, j, m) in enumerate(spots):
            count = taken(metas[1 + i, kk, j], b)
            keys.append(visible(jnp.broadcast_to(count, (page_rows, LANES)) > m, kv_mov[i, kk, j, m, 0]))
            used = jnp.where(count > m, 1.0, 0.0)
            hidden = hidden + (1.0 - used) * page_rows
            if n % along == 0:
                keep.append(used)
            else:
                keep[-1] = jnp.where(slot_lane >= n % along * page_rows, used, keep[-1])
        attend(
            jnp.concatenate(keys, axis=0),
            jnp.concatenate([kv_mov[i, kk, j, m, 1] for i, kk, j, m in spots], axis=0),
            jnp.concatenate(keep, axis=1).astype(jnp.bfloat16), hidden, None, False,
        )

    members = range(share)
    chips = range(kv_heads)
    slots = range(MOST)

    def relay_rows(j):
        arrived(kv_rn.at[0, j], r_rn.at[0, j])
        for k in range(1, share):
            start("rows", kv_rn.at[0, j], kv_rn.at[share - k, j], r_rn.at[share - k, j], b, peers[k])

    def peers_rows(j):
        for kk in range(1, share):
            arrived(kv_rn.at[kk, j], r_rn.at[kk, j])

    def relay_near(j):
        for k in range(near_count):
            arrived(kv_mov.at[k, 0, j], r_mov.at[k, j, 0])
            for p in range(1, share):
                start("pair", kv_mov.at[k, 0, j], kv_mov.at[k, share - p, j], r_peer.at[k, share - p - 1, j // 2], b, peers[p])

    def relay_far(e, j, m):
        i = near_count + e
        spot = kv_mov.at[i, 0, j, m]
        arrived(spot, r_mov.at[i, j, m])
        for p in range(1, share):
            start("page", spot, kv_mov.at[i, share - p, j, m], r_peer.at[i, share - p - 1, m], b, peers[p])

    def hub_relay(spots):
        @pl.when(is_hub)
        def _():
            for e, j in spots:
                i = near_count + e
                spot = kv_mov.at[i, 0, j, 1]
                arrived(spot, r_mov.at[i, j, 1])
                start("hub", spot, kv_mov.at[i, 0, j, 1], r_mov.at[i, j, 1], near(1), a)
                for p in range(1, share):
                    start("hub", spot, kv_mov.at[i, share - p, j, 1], r_peer.at[i, share - p - 1, 1], b, peers[p])

    def leaf_relay(spots):
        @pl.when(jnp.logical_not(is_hub))
        def _():
            for e, j in spots:
                i = near_count + e
                spot = kv_mov.at[i, 0, j, 1]
                arrived(spot, r_mov.at[i, j, 1])
                for p in range(1, share):
                    start("leaf", spot, kv_mov.at[i, share - p, j, 1], r_peer.at[i, share - p - 1, 1], b, peers[p])

    def send_metas():
        arrived(metas.at[0, 0, 1:kv_heads], r_meta.at[0, 0])
        block = metas.at[0, 0]
        for t in range(half):
            g = 1 + near_count + reach
            start("block", block, metas.at[g, 0], r_meta.at[g, 0], far(t), a)
        for k in range(1, half):
            start("block", block, metas.at[k, 0], r_meta.at[k, 0], near(k), a)

    def relay_metas():
        for g in range(1, groups):
            arrived(metas.at[g, 0], r_meta.at[g, 0])
            for p in range(1, share):
                start("block", metas.at[g, 0], metas.at[g, share - p], r_meta.at[1, share - p], b, peers[p])

    def peers_metas(lo, hi):
        for kk in range(1, share):
            arrived(metas.at[lo:hi, kk] if lo else metas.at[0, kk], r_meta.at[lo, kk])

    def attend_near(part):
        js = list(chips)[2 * part:2 * part + 2]
        for k in range(near_count):
            attend_moved([(k, kk, j, m) for j in js for kk in members for m in slots])

    def peers_near(part):
        js = list(chips)[2 * part:2 * part + 2]
        for k in range(near_count):
            for kk in range(1, share):
                arrived(kv_mov.at[k, kk, js[0]:js[-1] + 1], r_peer.at[k, kk - 1, part])

    def peers_far(e, m):
        i = near_count + e
        for kk in range(1, share):
            arrived(kv_mov.at[i, kk, :, m], r_peer.at[i, kk - 1, m])

    def attend_far(e, m):
        attend_moved([(near_count + e, kk, j, m) for j in chips for kk in members])

    others = range(1, kv_heads)
    late = [m for m in reversed(slots) if m == 0 or not shared]

    def relay_late(j):
        for e in range(half):
            for m in late:
                relay_far(e, j, m)

    send_on(1, 0)
    send_on(2, 0)
    peers_metas(0, 1)
    peers_rows(0)
    attend_resident([(kk, 0) for kk in members], True)
    send_on(3, 0)
    send_metas()
    send_on(1, 1)
    send_on(2, 1)
    send_on(3, 1)
    if shared:
        hub_relay([(0, 0), (1, 0), (0, 1), (0, 2)])
    relay_near(0)
    relay_late(0)
    relay_near(1)
    if shared:
        hub_relay([(0, 3), (1, 1), (1, 2)])
    relay_near(2)
    relay_near(3)
    relay_rows(1)
    relay_metas()
    relay_rows(2)
    if shared:
        hub_relay([(1, 3)])
    peers_near(0)
    peers_near(1)
    peers_metas(1, groups)
    attend_near(0)
    attend_near(1)
    relay_rows(3)
    relay_late(1)
    peers_rows(1)
    peers_rows(2)
    attend_resident([(kk, 1) for kk in members])
    attend_resident([(kk, 2) for kk in members])
    relay_late(2)
    peers_rows(3)
    relay_late(3)
    if shared:
        leaf_relay([(0, j) for j in chips])
    attend_resident([(kk, 3) for kk in members])
    attend_fresh()
    if shared:
        leaf_relay([(e, j) for e in range(1, half) for j in chips])
        peers_far(0, 1)
        peers_far(1, 1)
        attend_far(0, 1)
        attend_far(1, 1)
    for m in late:
        for e in range(half):
            peers_far(e, m)
    for m in late:
        for e in range(half):
            attend_far(e, m)

    def turn(h):
        part = slice(h * queries, (h + 1) * queries)
        return (run_out[:, part] / run_sum[:, part]).T

    for h in range(heads):
        out_ref[:, h * HEAD_DIM:(h + 1) * HEAD_DIM] = turn(h).astype(out_ref.dtype)

    for name in names:
        if name not in ("hub", "leaf"):
            all_left(name)
    for src, j, part in wide:
        remote(src, src, s_wide.at[j, part], s_load.at[0], b, a).wait_send()
    if shared:
        @pl.when(is_hub)
        def _():
            all_left("hub")

        @pl.when(jnp.logical_not(is_hub))
        def _():
            all_left("leaf")


def finish(append_ref, rows_ref, pool_ref, fresh_ref, out_ref, updated_ref):
    out_ref[...] = rows_ref[...]
    updated_ref[...] = pool_ref[...]
    updated_ref[append_ref[0, 0], 0:fresh_ref.shape[0]] = fresh_ref[...]


def local(n_inst, n_aa, queries, new_kv, pool, page_table, ctx_len, move_page, move_dest, append_page):
    pool_pages = pool[0]
    pages, page_rows, _, width = pool_pages.shape
    kv_heads = width // HEAD_DIM
    share = n_aa // kv_heads
    fresh_rows = new_kv[0]
    fresh_count = fresh_rows.shape[0]
    query_count, q_width = queries.shape[1:]
    heads = q_width // HEAD_DIM
    table = page_table.shape[1]
    moves = move_page.shape[1]
    half = n_inst // 2
    near = half - 1
    groups = 1 + near + half
    out_count = (near + half) * MOST
    per_kind = 3 if share < 4 else 9
    bf, f32 = jnp.bfloat16, jnp.float32
    dma = pltpu.SemaphoreType.DMA
    page = (2, page_rows, HEAD_DIM)
    rows = (2, fresh_count + table * page_rows, HEAD_DIM)
    attended = pl.pallas_call(
        functools.partial(kernel, n_inst, n_aa, kv_heads),
        out_shape=pltpu.VMEM((query_count, q_width), bf),
        in_specs=[pl.BlockSpec(memory_space=pltpu.HBM)] * 7,
        out_specs=pl.BlockSpec(memory_space=pltpu.VMEM),
        scratch_shapes=[
            *[pltpu.SMEM(x.shape, jnp.int32) for x in (page_table, ctx_len, move_page, move_dest)],
            pltpu.VMEM((query_count, q_width), bf),
            pltpu.VMEM(pool_pages.shape, bf),
            pltpu.VMEM(fresh_rows.shape, bf),
            pltpu.VMEM((moves, kv_heads, *page), bf),
            pltpu.VMEM((kv_heads, *rows), bf),
            pltpu.VMEM((kv_heads * out_count, *page), bf),
            pltpu.VMEM((kv_heads, out_count, *page), bf),
            pltpu.VMEM((near + half, share, kv_heads, MOST, *page), bf),
            pltpu.VMEM((share, kv_heads, *rows), bf),
            pltpu.VMEM((groups, share, kv_heads, 1, LANES), jnp.int32),
            pltpu.VMEM((1, heads * query_count), f32),
            pltpu.VMEM((1, heads * query_count), f32),
            pltpu.VMEM((1, heads * query_count), f32),
            pltpu.VMEM((HEAD_DIM, heads * query_count), f32),
            pltpu.VMEM((2 * HEAD_DIM, heads * query_count), bf),
            dma((7,)), dma((7, per_kind)),
            dma((share, kv_heads)), dma((near + half, kv_heads, MOST)), dma((near + half, share - 1, MOST)),
            dma((kv_heads, 2)), dma((groups, share)), dma((kv_heads, 2) if half > 2 else (1, 1)),
        ],
        compiler_params=pltpu.CompilerParams(collective_id=0, has_side_effects=True, vmem_limit_bytes=60 * 2**20),
        name="paged_attention",
    )(page_table, ctx_len, move_page, move_dest, queries[0], pool_pages, fresh_rows)
    attended, updated = pl.pallas_call(
        finish,
        out_shape=(
            jax.ShapeDtypeStruct(attended.shape, bf),
            jax.ShapeDtypeStruct(pool_pages.shape, bf),
        ),
        in_specs=[pl.BlockSpec(memory_space=pltpu.SMEM)] + [pl.BlockSpec(memory_space=pltpu.VMEM)] * 3,
        out_specs=(pl.BlockSpec(memory_space=pltpu.VMEM),) * 2,
        compiler_params=pltpu.CompilerParams(vmem_limit_bytes=12 * 2**20),
        name="finish",
    )(append_page, attended, pool_pages, fresh_rows)
    return (attended[None], updated[None])


def solution(mesh):
    return jax.shard_map(
        functools.partial(local, mesh.shape["ba"], mesh.shape["aa"]),
        mesh=mesh,
        in_specs=(
            P("ba", None, "aa"),
            P("ba", "aa", None, None),
            P("ba", "aa", None, None, None),
            P("ba", "aa"),
            P("ba", "aa"),
            P("ba", "aa"),
            P("ba", "aa"),
            P("ba", "aa"),
        ),
        out_specs=(P("ba", None, "aa"), P("ba", "aa", None, None, None)),
        check_vma=False,
    )
```

```python
import functools
import math

import jax
import jax.numpy as jnp
from jax import lax
from jax.experimental import pallas as pl
from jax.experimental.pallas import tpu as pltpu
from jax.sharding import PartitionSpec as P

HEAD_DIM = 128
MOST = 2
LANES = 128
BLOCK = 256
NEG_LARGE = -1e30
MESH = pl.DeviceIdType.MESH


def kernel(
    n_inst, n_aa, kv_heads,
    table_hbm, len_hbm, page_hbm, dest_hbm, q_hbm, pool_hbm, fresh_hbm,
    out_ref,
    table_ref, len_ref, page_ref, dest_ref, q_ref, pool_ref, fresh_ref,
    ext, st_rn, st_out, passed, kv_mov, kv_rn, metas,
    run_max, run_sum, spare_score, run_out, q_turned,
    s_load, s_all, r_rn, r_mov, r_peer, r_pass, r_meta, s_wide,
):
    b = lax.axis_index("ba")
    a = lax.axis_index("aa")
    share = n_aa // kv_heads
    mine, member = a // share, a % share
    half = n_inst // 2
    side = b // half
    base = side * half
    pos = b - base
    hub = half - 1 + side
    far_hub = half - side
    is_hub = b == hub
    reach = (1 - side) * (half - 1 - pos) + side * pos
    near_count = half - 1
    table = table_ref.shape[1]
    moves = page_ref.shape[1]
    page_rows = pool_ref.shape[1]
    fresh = fresh_ref.shape[0]
    queries = q_ref.shape[0]
    heads = q_ref.shape[1] // HEAD_DIM
    bits = (n_inst - 1).bit_length()
    shared = half == 2 and MOST == 2 and moves < 2 * MOST

    def near(k):
        return base + lax.rem(pos + k + half, half)

    def far(t):
        return far_hub + (1 - 2 * side) * t

    def flip(j):
        to = mine
        bit = 1
        while bit <= j:
            if j & bit:
                to = to + bit - 2 * bit * (mine // bit % 2)
            bit *= 2
        return to

    heads_at = [flip(j) for j in range(kv_heads)]
    device_at = [h * share + member for h in heads_at]
    peers = [mine * share + lax.rem(member + k, share) for k in range(share)]

    pool_load = pltpu.make_async_copy(pool_hbm, pool_ref, s_load.at[0])
    pool_load.start()
    q_load = pltpu.make_async_copy(q_hbm, q_ref, s_load.at[1])
    fresh_load = pltpu.make_async_copy(fresh_hbm, fresh_ref, s_load.at[2])
    small = []
    for n, (src, dst) in enumerate(((page_hbm, page_ref), (dest_hbm, dest_ref), (len_hbm, len_ref), (table_hbm, table_ref))):
        small.append(pltpu.make_async_copy(src, dst, s_load.at[3 + n]))
        small[-1].start()
    fresh_load.start()
    q_load.start()

    barrier = pltpu.get_barrier_semaphore()
    partners = [(b, device_at[j]) for j in range(1, kv_heads)]
    partners += [(b, peers[k]) for k in range(1, share)]
    partners += [(near(k), to) for k in range(1, half) for to in device_at]
    partners += [(far(t), a) for t in range(half)]
    for ba, aa in partners:
        pl.semaphore_signal(barrier, inc=1, device_id={"ba": ba, "aa": aa}, device_id_type=MESH)

    def columns_of(h):
        return slice(h * HEAD_DIM, (h + 1) * HEAD_DIM)

    for load in small:
        load.wait()
    code = len_ref[0, 0]
    for i in range(moves):
        code = code * (1 << bits) + dest_ref[0, i]
    metas[0, 0, 0] = jnp.full((1, LANES), code, jnp.int32)

    def chosen_for(target):
        seen = jnp.int32(0)
        picked = [jnp.int32(0) for _ in range(MOST)]
        for i in range(moves):
            hit = (dest_ref[0, i] == target).astype(jnp.int32)
            for m in range(MOST):
                picked[m] = picked[m] + hit * (seen == m).astype(jnp.int32) * i
            seen = seen + hit
        return picked, seen

    outs = [(0, t, m) for m in reversed(range(1, MOST)) for t in range(half) if not (shared and t)]
    first_cut = len(outs)
    outs += [(0, t, 0) for t in reversed(range(half))]
    second_cut = len(outs)
    outs += [(1, k, m) for k in range(1, half) for m in range(MOST)]
    cuts = [(0, first_cut), (first_cut, second_cut)]
    out_count = st_out.shape[0] // kv_heads

    pool_load.wait()
    for i in range(moves):
        turned = jnp.swapaxes(pool_ref[page_ref[0, i]], 0, 1)
        for h in range(kv_heads):
            ext[i, h] = turned[:, :, columns_of(h)]
    picked_far = [chosen_for(far(t)) for t in range(half)]
    picked_near = [chosen_for(near(k)) for k in range(half)]
    for n, (kind, t, m) in enumerate(outs):
        index = (picked_near if kind else picked_far)[t][0][m]
        if shared and not kind and m == 1:
            index = jnp.where(picked_far[0][1] > 1, index, picked_far[1][0][1])
        for h in range(kv_heads):
            st_out[h * out_count + n] = ext[index, h]

    def remote(src, dst, ss, rs, ba, aa):
        return pltpu.make_async_remote_copy(
            src_ref=src, dst_ref=dst, send_sem=ss, recv_sem=rs,
            device_id={"ba": ba, "aa": aa}, device_id_type=MESH,
        )

    groups = metas.shape[0]
    wide = []
    pages = st_out.shape[0]
    kinds = {
        "page": (pages, lambda r: st_out.at[0:r]),
        "hub": (pages, lambda r: st_out.at[0:r]),
        "leaf": (pages, lambda r: st_out.at[0:r]),
        "pair": (pages // MOST, lambda r: st_out.at[0:r * MOST]),
        "rows": (kv_heads, lambda r: st_rn.at[0:r]),
        "row": (kv_heads, lambda r: metas.at[0, 0, 0:r]),
        "block": (groups, lambda r: metas.at[0:r, 0]),
        "part": (groups, lambda r: metas.at[0:r, 0, 1:kv_heads]),
    }
    names = list(kinds)
    counts = {name: 0 for name in names}
    per_kind = s_all.shape[1]

    def start(kind, src, dst, rs, ba, aa):
        n = counts[kind] // kinds[kind][0]
        assert n < per_kind
        counts[kind] += 1
        remote(src, dst, s_all.at[names.index(kind), n], rs, ba, aa).start()

    def all_left(kind):
        size, piece = kinds[kind]
        for n in range(0, counts[kind], size):
            ref = piece(min(size, counts[kind] - n))
            remote(ref, ref, s_all.at[names.index(kind), n // size], s_load.at[0], b, a).wait_send()

    def arrived(slot, rs):
        remote(slot, slot, s_load.at[0], rs, b, a).wait_recv()

    def shifted(row, count):
        return lax.shift_right_logical(row, jnp.full(row.shape, count, jnp.int32))

    def taken(row, target):
        low = jnp.full(row.shape, (1 << bits) - 1, jnp.int32)
        count = jnp.zeros(row.shape, jnp.int32)
        for i in range(moves):
            dest = lax.bitwise_and(shifted(row, bits * (moves - 1 - i)), low)
            count = count + (dest == target).astype(jnp.int32)
        return count

    fresh_load.wait()
    for lo, block in [(0, 0)] + [(fresh + i * page_rows, i) for i in range(table)]:
        turned = jnp.swapaxes(fresh_ref[...] if lo == 0 else pool_ref[table_ref[0, block]], 0, 1)
        for h in range(kv_heads):
            st_rn[h, :, lo:lo + turned.shape[1], :] = turned[:, :, columns_of(h)]
    pl.semaphore_wait(barrier, len(partners))

    def source(j, lo, hi):
        return st_out.at[pl.ds(mine * out_count + lo, hi - lo)] if j == 0 else passed.at[j, lo:hi]

    def send_on(j, part):
        lo, hi = cuts[part]
        if j:
            arrived(passed.at[j, lo:hi], r_pass.at[j, part])
        i = near_count + reach
        for n in range(lo, hi):
            _, t, m = outs[n]
            start("page", source(j, n, n + 1), kv_mov.at[i, 0, j, m:m + 1], r_mov.at[i, j, m], far(t), a)

    def send_near(j):
        for k in range(1, half):
            n = second_cut + (k - 1) * MOST
            start("pair", st_out.at[pl.ds(heads_at[j] * out_count + n, MOST)], kv_mov.at[k - 1, 0, j], r_mov.at[k - 1, j, 0], near(k), device_at[j])

    def send_plane(j, part):
        lo, hi = cuts[part]
        kind = {1: "page", 2: "pair"}
        src, dst = st_out.at[pl.ds(heads_at[j] * out_count + lo, hi - lo)], passed.at[j, lo:hi]
        if hi - lo in kind:
            start(kind[hi - lo], src, dst, r_pass.at[j, part], b, device_at[j])
        else:
            wide.append((src, j, part))
            remote(src, dst, s_wide.at[j, part], r_pass.at[j, part], b, device_at[j]).start()

    send_on(0, 0)
    for j in range(1, kv_heads):
        send_plane(j, 0)
    send_on(0, 1)
    for j in range(1, kv_heads):
        start("row", metas.at[0, 0, 0], metas.at[0, 0, j], r_meta.at[0, 0], b, device_at[j])
    for k in range(1, share):
        start("row", metas.at[0, 0, 0], metas.at[0, share - k, 0], r_meta.at[0, share - k], b, peers[k])
    for j in range(kv_heads):
        send_near(j)
    for j in range(1, kv_heads):
        send_plane(j, 1)
    for k in range(1, share):
        start("rows", st_rn.at[mine], kv_rn.at[share - k, 0], r_rn.at[share - k, 0], b, peers[k])
    for j in range(1, kv_heads):
        start("rows", st_rn.at[heads_at[j]], kv_rn.at[0, j], r_rn.at[0, j], b, device_at[j])

    q_load.wait()
    scale = math.log2(math.e) / math.sqrt(HEAD_DIM)
    for h in range(heads):
        part = slice(h * queries, (h + 1) * queries)
        turned = q_ref[:, h * HEAD_DIM:(h + 1) * HEAD_DIM].T.astype(jnp.float32) * scale
        high = turned.astype(jnp.bfloat16)
        q_turned[0:HEAD_DIM, part] = high
        q_turned[HEAD_DIM:2 * HEAD_DIM, part] = (turned - high.astype(jnp.float32)).astype(jnp.bfloat16)

    def attend(keys, values, keep, hidden, bias, first):
        left = values.T
        if bias is None:
            left = left * keep
            hidden = jnp.concatenate([hidden] * (BLOCK // LANES), axis=1)
        else:
            bias = jnp.concatenate([bias] * (BLOCK // bias.shape[1]), axis=1)
        both = jnp.concatenate([keys, keys], axis=1)
        for start_at in range(0, heads * queries, BLOCK):
            block = slice(start_at, start_at + BLOCK)
            s = jnp.dot(both, q_turned[:, block], preferred_element_type=jnp.float32)
            if bias is not None:
                s = s + bias
            top = jnp.max(s, axis=0, keepdims=True)
            if not first:
                old = run_max[:, block]
                top = jnp.maximum(old, top)
            w = jnp.exp2(s - top)
            total = jnp.sum(w, axis=0, keepdims=True)
            if bias is None:
                total = total - hidden * jnp.exp2(spare_score[:, block] - top)
            high = w.astype(jnp.bfloat16)
            low = (w - high.astype(jnp.float32)).astype(jnp.bfloat16)
            out = jnp.dot(left, high, preferred_element_type=jnp.float32)
            out = out + jnp.dot(left, low, preferred_element_type=jnp.float32)
            if not first:
                shrink = jnp.exp2(old - top)
                total = total + run_sum[:, block] * shrink
                out = out + run_out[:, block] * shrink
            run_max[:, block] = top
            run_sum[:, block] = total
            run_out[:, block] = out

    def rows_of(kk, j):
        return st_rn.at[mine] if kk == 0 and j == 0 else kv_rn.at[kk, j]

    chunk = table * page_rows
    place = lax.broadcasted_iota(jnp.int32, (chunk, LANES), 0)
    lane = lax.broadcasted_iota(jnp.int32, (1, chunk), 1)
    slot_lane = lax.broadcasted_iota(jnp.int32, (1, LANES), 1)
    spare = st_rn[mine, 0, fresh:fresh + 16, :]
    for start_at in range(0, heads * queries, BLOCK):
        block = slice(start_at, start_at + BLOCK)
        spare_score[:, block] = jnp.dot(
            jnp.concatenate([spare, spare], axis=1), q_turned[:, block], preferred_element_type=jnp.float32
        )[0:1]
    spare = spare[0:1].astype(jnp.float32)

    def visible(mask, keys):
        return jnp.where(mask, keys.astype(jnp.float32), spare).astype(jnp.bfloat16)

    def attend_resident(spots, first=False):
        keys, values, keep = [], [], []
        hidden = jnp.zeros((1, LANES), jnp.int32)
        for kk, j in spots:
            live = shifted(metas[0, kk, j], bits * moves)
            rows = rows_of(kk, j)
            keys.append(visible(place < live, rows[0, fresh:]))
            values.append(rows[1, fresh:])
            wide_live = jnp.concatenate([live] * (chunk // LANES), axis=1)
            keep.append(jnp.where(lane < wide_live, 1.0, 0.0))
            hidden = hidden + (chunk - live)
        attend(
            jnp.concatenate(keys, axis=0), jnp.concatenate(values, axis=0),
            jnp.concatenate(keep, axis=1).astype(jnp.bfloat16), hidden.astype(jnp.float32), None, first,
        )

    def attend_fresh():
        spots = [(kk, j) for j in range(kv_heads) for kk in range(share)]
        line = lax.broadcasted_iota(jnp.int32, (fresh, queries), 0)
        column = lax.broadcasted_iota(jnp.int32, (fresh, queries), 1)
        biases = []
        for kk, j in spots:
            owner = heads_at[j] * share + lax.rem(member + kk, share)
            biases.append(jnp.where(line + owner * fresh <= column, 0.0, NEG_LARGE))
        attend(
            jnp.concatenate([rows_of(kk, j)[0, :fresh] for kk, j in spots], axis=0),
            jnp.concatenate([rows_of(kk, j)[1, :fresh] for kk, j in spots], axis=0),
            None, None, jnp.concatenate(biases, axis=0), False,
        )

    def attend_moved(spots):
        along = LANES // page_rows
        keys, keep = [], []
        hidden = jnp.zeros((1, LANES), jnp.float32)
        for n, (i, kk, j, m) in enumerate(spots):
            count = taken(metas[1 + i, kk, j], b)
            keys.append(visible(jnp.broadcast_to(count, (page_rows, LANES)) > m, kv_mov[i, kk, j, m, 0]))
            used = jnp.where(count > m, 1.0, 0.0)
            hidden = hidden + (1.0 - used) * page_rows
            if n % along == 0:
                keep.append(used)
            else:
                keep[-1] = jnp.where(slot_lane >= n % along * page_rows, used, keep[-1])
        attend(
            jnp.concatenate(keys, axis=0),
            jnp.concatenate([kv_mov[i, kk, j, m, 1] for i, kk, j, m in spots], axis=0),
            jnp.concatenate(keep, axis=1).astype(jnp.bfloat16), hidden, None, False,
        )

    members = range(share)
    chips = range(kv_heads)
    slots = range(MOST)

    def relay_rows(j):
        arrived(kv_rn.at[0, j], r_rn.at[0, j])
        for k in range(1, share):
            start("rows", kv_rn.at[0, j], kv_rn.at[share - k, j], r_rn.at[share - k, j], b, peers[k])

    def peers_rows(j):
        for kk in range(1, share):
            arrived(kv_rn.at[kk, j], r_rn.at[kk, j])

    def relay_near(j):
        for k in range(near_count):
            arrived(kv_mov.at[k, 0, j], r_mov.at[k, j, 0])
            for p in range(1, share):
                start("pair", kv_mov.at[k, 0, j], kv_mov.at[k, share - p, j], r_peer.at[k, share - p - 1, j // 2], b, peers[p])

    def relay_far(e, j, m):
        i = near_count + e
        spot = kv_mov.at[i, 0, j, m]
        arrived(spot, r_mov.at[i, j, m])
        for p in range(1, share):
            start("page", spot, kv_mov.at[i, share - p, j, m], r_peer.at[i, share - p - 1, m], b, peers[p])

    def hub_relay(spots):
        @pl.when(is_hub)
        def _():
            for e, j in spots:
                i = near_count + e
                spot = kv_mov.at[i, 0, j, 1]
                arrived(spot, r_mov.at[i, j, 1])
                start("hub", spot, kv_mov.at[i, 0, j, 1], r_mov.at[i, j, 1], near(1), a)
                for p in range(1, share):
                    start("hub", spot, kv_mov.at[i, share - p, j, 1], r_peer.at[i, share - p - 1, 1], b, peers[p])

    def leaf_relay(spots):
        @pl.when(jnp.logical_not(is_hub))
        def _():
            for e, j in spots:
                i = near_count + e
                spot = kv_mov.at[i, 0, j, 1]
                arrived(spot, r_mov.at[i, j, 1])
                for p in range(1, share):
                    start("leaf", spot, kv_mov.at[i, share - p, j, 1], r_peer.at[i, share - p - 1, 1], b, peers[p])

    def send_metas():
        arrived(metas.at[0, 0, 1:kv_heads], r_meta.at[0, 0])
        block = metas.at[0, 0]
        for t in range(half):
            g = 1 + near_count + reach
            start("block", block, metas.at[g, 0], r_meta.at[g, 0], far(t), a)
        for k in range(1, half):
            start("block", block, metas.at[k, 0], r_meta.at[k, 0], near(k), a)
        for p in range(1, share):
            start("part", metas.at[0, 0, 1:kv_heads], metas.at[0, share - p, 1:kv_heads], r_meta.at[groups, share - p], b, peers[p])

    def relay_metas(lo, hi):
        for g in range(lo, hi):
            arrived(metas.at[g, 0], r_meta.at[g, 0])
            for p in range(1, share):
                start("block", metas.at[g, 0], metas.at[g, share - p], r_meta.at[lo, share - p], b, peers[p])

    def peers_own_row():
        for kk in range(1, share):
            arrived(metas.at[0, kk, 0], r_meta.at[0, kk])

    def peers_plane():
        for kk in range(1, share):
            arrived(metas.at[0, kk, 1:kv_heads], r_meta.at[groups, kk])

    def peers_metas(lo, hi):
        for kk in range(1, share):
            arrived(metas.at[lo:hi, kk], r_meta.at[lo, kk])

    def attend_near(part):
        js = list(chips)[2 * part:2 * part + 2]
        for k in range(near_count):
            attend_moved([(k, kk, j, m) for j in js for kk in members for m in slots])

    def peers_near(part):
        js = list(chips)[2 * part:2 * part + 2]
        for k in range(near_count):
            for kk in range(1, share):
                arrived(kv_mov.at[k, kk, js[0]:js[-1] + 1], r_peer.at[k, kk - 1, part])

    def peers_far(e, m):
        i = near_count + e
        for kk in range(1, share):
            arrived(kv_mov.at[i, kk, :, m], r_peer.at[i, kk - 1, m])

    def attend_far(e, m):
        attend_moved([(near_count + e, kk, j, m) for j in chips for kk in members])

    others = range(1, kv_heads)
    late = [m for m in reversed(slots) if m == 0 or not shared]

    def relay_late(j):
        for e in range(half):
            for m in late:
                relay_far(e, j, m)

    send_on(1, 0)
    send_on(2, 0)
    peers_own_row()
    peers_rows(0)
    attend_resident([(kk, 0) for kk in members], True)
    send_on(3, 0)
    send_metas()
    send_on(1, 1)
    send_on(2, 1)
    send_on(3, 1)
    first_far = 1 + near_count
    if shared:
        hub_relay([(0, 0), (1, 0), (0, 1)])
    if near_count:
        relay_metas(1, first_far)
    relay_near(0)
    relay_near(1)
    relay_late(0)
    if shared:
        hub_relay([(0, 2), (0, 3)])
    if near_count:
        peers_metas(1, first_far)
    peers_near(0)
    attend_near(0)
    relay_near(2)
    relay_near(3)
    if shared:
        hub_relay([(1, 1), (1, 2)])
    relay_rows(1)
    relay_rows(2)
    peers_near(1)
    attend_near(1)
    relay_rows(3)
    if shared:
        hub_relay([(1, 3)])
    relay_late(1)
    peers_plane()
    peers_rows(1)
    peers_rows(2)
    attend_resident([(kk, 1) for kk in members])
    attend_resident([(kk, 2) for kk in members])
    relay_late(2)
    relay_metas(first_far, groups)
    relay_late(3)
    if shared:
        leaf_relay([(0, j) for j in chips])
    peers_rows(3)
    attend_resident([(kk, 3) for kk in members])
    attend_fresh()
    if shared:
        leaf_relay([(e, j) for e in range(1, half) for j in chips])
    peers_metas(first_far, groups)
    for e in range(half):
        for m in reversed(slots):
            peers_far(e, m)
        for m in reversed(slots):
            attend_far(e, m)

    def turn(h):
        part = slice(h * queries, (h + 1) * queries)
        return (run_out[:, part] / run_sum[:, part]).T

    for h in range(heads):
        out_ref[:, h * HEAD_DIM:(h + 1) * HEAD_DIM] = turn(h).astype(out_ref.dtype)

    for name in names:
        if name not in ("hub", "leaf"):
            all_left(name)
    for src, j, part in wide:
        remote(src, src, s_wide.at[j, part], s_load.at[0], b, a).wait_send()
    if shared:
        @pl.when(is_hub)
        def _():
            all_left("hub")

        @pl.when(jnp.logical_not(is_hub))
        def _():
            all_left("leaf")


def finish(append_ref, rows_ref, pool_ref, fresh_ref, out_ref, updated_ref):
    out_ref[...] = rows_ref[...]
    updated_ref[...] = pool_ref[...]
    updated_ref[append_ref[0, 0], 0:fresh_ref.shape[0]] = fresh_ref[...]


def local(n_inst, n_aa, queries, new_kv, pool, page_table, ctx_len, move_page, move_dest, append_page):
    pool_pages = pool[0]
    pages, page_rows, _, width = pool_pages.shape
    kv_heads = width // HEAD_DIM
    share = n_aa // kv_heads
    fresh_rows = new_kv[0]
    fresh_count = fresh_rows.shape[0]
    query_count, q_width = queries.shape[1:]
    heads = q_width // HEAD_DIM
    table = page_table.shape[1]
    moves = move_page.shape[1]
    half = n_inst // 2
    near = half - 1
    groups = 1 + near + half
    out_count = (near + half) * MOST
    per_kind = 3 if share < 4 else 9
    bf, f32 = jnp.bfloat16, jnp.float32
    dma = pltpu.SemaphoreType.DMA
    page = (2, page_rows, HEAD_DIM)
    rows = (2, fresh_count + table * page_rows, HEAD_DIM)
    attended = pl.pallas_call(
        functools.partial(kernel, n_inst, n_aa, kv_heads),
        out_shape=pltpu.VMEM((query_count, q_width), bf),
        in_specs=[pl.BlockSpec(memory_space=pltpu.HBM)] * 7,
        out_specs=pl.BlockSpec(memory_space=pltpu.VMEM),
        scratch_shapes=[
            *[pltpu.SMEM(x.shape, jnp.int32) for x in (page_table, ctx_len, move_page, move_dest)],
            pltpu.VMEM((query_count, q_width), bf),
            pltpu.VMEM(pool_pages.shape, bf),
            pltpu.VMEM(fresh_rows.shape, bf),
            pltpu.VMEM((moves, kv_heads, *page), bf),
            pltpu.VMEM((kv_heads, *rows), bf),
            pltpu.VMEM((kv_heads * out_count, *page), bf),
            pltpu.VMEM((kv_heads, out_count, *page), bf),
            pltpu.VMEM((near + half, share, kv_heads, MOST, *page), bf),
            pltpu.VMEM((share, kv_heads, *rows), bf),
            pltpu.VMEM((groups, share, kv_heads, 1, LANES), jnp.int32),
            pltpu.VMEM((1, heads * query_count), f32),
            pltpu.VMEM((1, heads * query_count), f32),
            pltpu.VMEM((1, heads * query_count), f32),
            pltpu.VMEM((HEAD_DIM, heads * query_count), f32),
            pltpu.VMEM((2 * HEAD_DIM, heads * query_count), bf),
            dma((7,)), dma((8, per_kind)),
            dma((share, kv_heads)), dma((near + half, kv_heads, MOST)), dma((near + half, share - 1, MOST)),
            dma((kv_heads, 2)), dma((groups + 1, share)), dma((kv_heads, 2) if half > 2 else (1, 1)),
        ],
        compiler_params=pltpu.CompilerParams(collective_id=0, has_side_effects=True, vmem_limit_bytes=60 * 2**20),
        name="paged_attention",
    )(page_table, ctx_len, move_page, move_dest, queries[0], pool_pages, fresh_rows)
    attended, updated = pl.pallas_call(
        finish,
        out_shape=(
            jax.ShapeDtypeStruct(attended.shape, bf),
            jax.ShapeDtypeStruct(pool_pages.shape, bf),
        ),
        in_specs=[pl.BlockSpec(memory_space=pltpu.SMEM)] + [pl.BlockSpec(memory_space=pltpu.VMEM)] * 3,
        out_specs=(pl.BlockSpec(memory_space=pltpu.VMEM),) * 2,
        compiler_params=pltpu.CompilerParams(vmem_limit_bytes=12 * 2**20),
        name="finish",
    )(append_page, attended, pool_pages, fresh_rows)
    return (attended[None], updated[None])


def solution(mesh):
    return jax.shard_map(
        functools.partial(local, mesh.shape["ba"], mesh.shape["aa"]),
        mesh=mesh,
        in_specs=(
            P("ba", None, "aa"),
            P("ba", "aa", None, None),
            P("ba", "aa", None, None, None),
            P("ba", "aa"),
            P("ba", "aa"),
            P("ba", "aa"),
            P("ba", "aa"),
            P("ba", "aa"),
        ),
        out_specs=(P("ba", None, "aa"), P("ba", "aa", None, None, None)),
        check_vma=False,
    )
```

```python
import functools
import math

import jax
import jax.numpy as jnp
from jax import lax
from jax.experimental import pallas as pl
from jax.experimental.pallas import tpu as pltpu
from jax.sharding import PartitionSpec as P

HEAD_DIM = 128
MOST = 2
LANES = 128
BLOCK = 256
NEG_LARGE = -1e30
MESH = pl.DeviceIdType.MESH


def kernel(
    n_inst, n_aa, kv_heads,
    table_hbm, len_hbm, page_hbm, dest_hbm, q_hbm, pool_hbm, fresh_hbm,
    out_ref,
    table_ref, len_ref, page_ref, dest_ref, q_ref, pool_ref, fresh_ref,
    ext, st_rn, st_out, passed, kv_mov, kv_rn, metas,
    run_max, run_sum, spare_score, run_out, q_turned,
    s_load, s_all, r_rn, r_mov, r_peer, r_pass, r_meta, s_wide,
):
    b = lax.axis_index("ba")
    a = lax.axis_index("aa")
    share = n_aa // kv_heads
    mine, member = a // share, a % share
    half = n_inst // 2
    side = b // half
    base = side * half
    pos = b - base
    hub = half - 1 + side
    far_hub = half - side
    is_hub = b == hub
    reach = (1 - side) * (half - 1 - pos) + side * pos
    near_count = half - 1
    table = table_ref.shape[1]
    moves = page_ref.shape[1]
    page_rows = pool_ref.shape[1]
    fresh = fresh_ref.shape[0]
    queries = q_ref.shape[0]
    heads = q_ref.shape[1] // HEAD_DIM
    bits = (n_inst - 1).bit_length()
    shared = half == 2 and MOST == 2 and moves < 2 * MOST

    def near(k):
        return base + lax.rem(pos + k + half, half)

    def far(t):
        return far_hub + (1 - 2 * side) * t

    def flip(j):
        to = mine
        bit = 1
        while bit <= j:
            if j & bit:
                to = to + bit - 2 * bit * (mine // bit % 2)
            bit *= 2
        return to

    heads_at = [flip(j) for j in range(kv_heads)]
    device_at = [h * share + member for h in heads_at]
    peers = [mine * share + lax.rem(member + k, share) for k in range(share)]

    pool_load = pltpu.make_async_copy(pool_hbm, pool_ref, s_load.at[0])
    pool_load.start()
    q_load = pltpu.make_async_copy(q_hbm, q_ref, s_load.at[1])
    fresh_load = pltpu.make_async_copy(fresh_hbm, fresh_ref, s_load.at[2])
    small = []
    for n, (src, dst) in enumerate(((page_hbm, page_ref), (dest_hbm, dest_ref), (len_hbm, len_ref), (table_hbm, table_ref))):
        small.append(pltpu.make_async_copy(src, dst, s_load.at[3 + n]))
        small[-1].start()
    fresh_load.start()
    q_load.start()

    barrier = pltpu.get_barrier_semaphore()
    partners = [(b, device_at[j]) for j in range(1, kv_heads)]
    partners += [(b, peers[k]) for k in range(1, share)]
    partners += [(near(k), to) for k in range(1, half) for to in device_at]
    partners += [(far(t), a) for t in range(half)]
    for ba, aa in partners:
        pl.semaphore_signal(barrier, inc=1, device_id={"ba": ba, "aa": aa}, device_id_type=MESH)

    def columns_of(h):
        return slice(h * HEAD_DIM, (h + 1) * HEAD_DIM)

    for load in small:
        load.wait()
    code = len_ref[0, 0]
    for i in range(moves):
        code = code * (1 << bits) + dest_ref[0, i]
    metas[0, 0, 0] = jnp.full((1, LANES), code, jnp.int32)

    def chosen_for(target):
        seen = jnp.int32(0)
        picked = [jnp.int32(0) for _ in range(MOST)]
        for i in range(moves):
            hit = (dest_ref[0, i] == target).astype(jnp.int32)
            for m in range(MOST):
                picked[m] = picked[m] + hit * (seen == m).astype(jnp.int32) * i
            seen = seen + hit
        return picked, seen

    outs = [(0, t, m) for m in reversed(range(1, MOST)) for t in range(half) if not (shared and t)]
    first_cut = len(outs)
    outs += [(0, t, 0) for t in reversed(range(half))]
    second_cut = len(outs)
    outs += [(1, k, m) for k in range(1, half) for m in range(MOST)]
    cuts = [(0, first_cut), (first_cut, second_cut)]
    out_count = st_out.shape[0] // kv_heads

    pool_load.wait()
    for i in range(moves):
        turned = jnp.swapaxes(pool_ref[page_ref[0, i]], 0, 1)
        for h in range(kv_heads):
            ext[i, h] = turned[:, :, columns_of(h)]
    picked_far = [chosen_for(far(t)) for t in range(half)]
    picked_near = [chosen_for(near(k)) for k in range(half)]
    for n, (kind, t, m) in enumerate(outs):
        index = (picked_near if kind else picked_far)[t][0][m]
        if shared and not kind and m == 1:
            index = jnp.where(picked_far[0][1] > 1, index, picked_far[1][0][1])
        for h in range(kv_heads):
            st_out[h * out_count + n] = ext[index, h]

    def remote(src, dst, ss, rs, ba, aa):
        return pltpu.make_async_remote_copy(
            src_ref=src, dst_ref=dst, send_sem=ss, recv_sem=rs,
            device_id={"ba": ba, "aa": aa}, device_id_type=MESH,
        )

    groups = metas.shape[0]
    wide = []
    pages = st_out.shape[0]
    kinds = {
        "page": (pages, lambda r: st_out.at[0:r]),
        "hub": (pages, lambda r: st_out.at[0:r]),
        "leaf": (pages, lambda r: st_out.at[0:r]),
        "pair": (pages // MOST, lambda r: st_out.at[0:r * MOST]),
        "rows": (kv_heads, lambda r: st_rn.at[0:r]),
        "row": (kv_heads, lambda r: metas.at[0, 0, 0:r]),
        "block": (groups, lambda r: metas.at[0:r, 0]),
        "part": (groups, lambda r: metas.at[0:r, 0, 1:kv_heads]),
    }
    names = list(kinds)
    counts = {name: 0 for name in names}
    per_kind = s_all.shape[1]

    def start(kind, src, dst, rs, ba, aa):
        n = counts[kind] // kinds[kind][0]
        assert n < per_kind
        counts[kind] += 1
        remote(src, dst, s_all.at[names.index(kind), n], rs, ba, aa).start()

    def all_left(kind):
        size, piece = kinds[kind]
        for n in range(0, counts[kind], size):
            ref = piece(min(size, counts[kind] - n))
            remote(ref, ref, s_all.at[names.index(kind), n // size], s_load.at[0], b, a).wait_send()

    def arrived(slot, rs):
        remote(slot, slot, s_load.at[0], rs, b, a).wait_recv()

    def shifted(row, count):
        return lax.shift_right_logical(row, jnp.full(row.shape, count, jnp.int32))

    def taken(row, target):
        low = jnp.full(row.shape, (1 << bits) - 1, jnp.int32)
        count = jnp.zeros(row.shape, jnp.int32)
        for i in range(moves):
            dest = lax.bitwise_and(shifted(row, bits * (moves - 1 - i)), low)
            count = count + (dest == target).astype(jnp.int32)
        return count

    fresh_load.wait()
    for lo, block in [(0, 0)] + [(fresh + i * page_rows, i) for i in range(table)]:
        turned = jnp.swapaxes(fresh_ref[...] if lo == 0 else pool_ref[table_ref[0, block]], 0, 1)
        for h in range(kv_heads):
            st_rn[h, :, lo:lo + turned.shape[1], :] = turned[:, :, columns_of(h)]
    pl.semaphore_wait(barrier, len(partners))

    def source(j, lo, hi):
        return st_out.at[pl.ds(mine * out_count + lo, hi - lo)] if j == 0 else passed.at[j, lo:hi]

    def send_on(j, part):
        lo, hi = cuts[part]
        if j:
            arrived(passed.at[j, lo:hi], r_pass.at[j, part])
        i = near_count + reach
        for n in range(lo, hi):
            _, t, m = outs[n]
            start("page", source(j, n, n + 1), kv_mov.at[i, 0, j, m:m + 1], r_mov.at[i, j, m], far(t), a)

    def send_near(j):
        for k in range(1, half):
            n = second_cut + (k - 1) * MOST
            start("pair", st_out.at[pl.ds(heads_at[j] * out_count + n, MOST)], kv_mov.at[k - 1, 0, j], r_mov.at[k - 1, j, 0], near(k), device_at[j])

    def send_plane(j, part):
        lo, hi = cuts[part]
        kind = {1: "page", 2: "pair"}
        src, dst = st_out.at[pl.ds(heads_at[j] * out_count + lo, hi - lo)], passed.at[j, lo:hi]
        if hi - lo in kind:
            start(kind[hi - lo], src, dst, r_pass.at[j, part], b, device_at[j])
        else:
            wide.append((src, j, part))
            remote(src, dst, s_wide.at[j, part], r_pass.at[j, part], b, device_at[j]).start()

    send_on(0, 0)
    for j in range(1, kv_heads):
        send_plane(j, 0)
    send_on(0, 1)
    for j in range(1, kv_heads):
        start("row", metas.at[0, 0, 0], metas.at[0, 0, j], r_meta.at[0, 0], b, device_at[j])
    for k in range(1, share):
        start("row", metas.at[0, 0, 0], metas.at[0, share - k, 0], r_meta.at[0, share - k], b, peers[k])
    for j in range(kv_heads):
        send_near(j)
    for j in range(1, kv_heads):
        send_plane(j, 1)
    for k in range(1, share):
        start("rows", st_rn.at[mine], kv_rn.at[share - k, 0], r_rn.at[share - k, 0], b, peers[k])
    for j in range(1, kv_heads):
        start("rows", st_rn.at[heads_at[j]], kv_rn.at[0, j], r_rn.at[0, j], b, device_at[j])

    q_load.wait()
    scale = math.log2(math.e) / math.sqrt(HEAD_DIM)
    for h in range(heads):
        part = slice(h * queries, (h + 1) * queries)
        turned = q_ref[:, h * HEAD_DIM:(h + 1) * HEAD_DIM].T.astype(jnp.float32) * scale
        high = turned.astype(jnp.bfloat16)
        q_turned[0:HEAD_DIM, part] = high
        q_turned[HEAD_DIM:2 * HEAD_DIM, part] = (turned - high.astype(jnp.float32)).astype(jnp.bfloat16)

    def attend(keys, values, keep, hidden, bias, first):
        left = values.T
        if bias is None:
            left = left * keep
            hidden = jnp.concatenate([hidden] * (BLOCK // LANES), axis=1)
        else:
            bias = jnp.concatenate([bias] * (BLOCK // bias.shape[1]), axis=1)
        both = jnp.concatenate([keys, keys], axis=1)
        for start_at in range(0, heads * queries, BLOCK):
            block = slice(start_at, start_at + BLOCK)
            s = jnp.dot(both, q_turned[:, block], preferred_element_type=jnp.float32)
            if bias is not None:
                s = s + bias
            top = jnp.max(s, axis=0, keepdims=True)
            if not first:
                old = run_max[:, block]
                top = jnp.maximum(old, top)
            w = jnp.exp2(s - top)
            total = jnp.sum(w, axis=0, keepdims=True)
            if bias is None:
                total = total - hidden * jnp.exp2(spare_score[:, block] - top)
            high = w.astype(jnp.bfloat16)
            low = (w - high.astype(jnp.float32)).astype(jnp.bfloat16)
            out = jnp.dot(left, high, preferred_element_type=jnp.float32)
            out = out + jnp.dot(left, low, preferred_element_type=jnp.float32)
            if not first:
                shrink = jnp.exp2(old - top)
                total = total + run_sum[:, block] * shrink
                out = out + run_out[:, block] * shrink
            run_max[:, block] = top
            run_sum[:, block] = total
            run_out[:, block] = out

    def rows_of(kk, j):
        return st_rn.at[mine] if kk == 0 and j == 0 else kv_rn.at[kk, j]

    chunk = table * page_rows
    place = lax.broadcasted_iota(jnp.int32, (chunk, LANES), 0)
    lane = lax.broadcasted_iota(jnp.int32, (1, chunk), 1)
    slot_lane = lax.broadcasted_iota(jnp.int32, (1, LANES), 1)
    spare = st_rn[mine, 0, fresh:fresh + 16, :]
    for start_at in range(0, heads * queries, BLOCK):
        block = slice(start_at, start_at + BLOCK)
        spare_score[:, block] = jnp.dot(
            jnp.concatenate([spare, spare], axis=1), q_turned[:, block], preferred_element_type=jnp.float32
        )[0:1]
    spare = spare[0:1].astype(jnp.float32)

    def visible(mask, keys):
        return jnp.where(mask, keys.astype(jnp.float32), spare).astype(jnp.bfloat16)

    def attend_resident(spots, first=False):
        keys, values, keep = [], [], []
        hidden = jnp.zeros((1, LANES), jnp.int32)
        for kk, j in spots:
            live = shifted(metas[0, kk, j], bits * moves)
            rows = rows_of(kk, j)
            keys.append(visible(place < live, rows[0, fresh:]))
            values.append(rows[1, fresh:])
            wide_live = jnp.concatenate([live] * (chunk // LANES), axis=1)
            keep.append(jnp.where(lane < wide_live, 1.0, 0.0))
            hidden = hidden + (chunk - live)
        attend(
            jnp.concatenate(keys, axis=0), jnp.concatenate(values, axis=0),
            jnp.concatenate(keep, axis=1).astype(jnp.bfloat16), hidden.astype(jnp.float32), None, first,
        )

    def attend_fresh():
        spots = [(kk, j) for j in range(kv_heads) for kk in range(share)]
        line = lax.broadcasted_iota(jnp.int32, (fresh, queries), 0)
        column = lax.broadcasted_iota(jnp.int32, (fresh, queries), 1)
        biases = []
        for kk, j in spots:
            owner = heads_at[j] * share + lax.rem(member + kk, share)
            biases.append(jnp.where(line + owner * fresh <= column, 0.0, NEG_LARGE))
        attend(
            jnp.concatenate([rows_of(kk, j)[0, :fresh] for kk, j in spots], axis=0),
            jnp.concatenate([rows_of(kk, j)[1, :fresh] for kk, j in spots], axis=0),
            None, None, jnp.concatenate(biases, axis=0), False,
        )

    def attend_moved(spots):
        along = LANES // page_rows
        keys, keep = [], []
        hidden = jnp.zeros((1, LANES), jnp.float32)
        for n, (i, kk, j, m) in enumerate(spots):
            count = taken(metas[1 + i, kk, j], b)
            keys.append(visible(jnp.broadcast_to(count, (page_rows, LANES)) > m, kv_mov[i, kk, j, m, 0]))
            used = jnp.where(count > m, 1.0, 0.0)
            hidden = hidden + (1.0 - used) * page_rows
            if n % along == 0:
                keep.append(used)
            else:
                keep[-1] = jnp.where(slot_lane >= n % along * page_rows, used, keep[-1])
        attend(
            jnp.concatenate(keys, axis=0),
            jnp.concatenate([kv_mov[i, kk, j, m, 1] for i, kk, j, m in spots], axis=0),
            jnp.concatenate(keep, axis=1).astype(jnp.bfloat16), hidden, None, False,
        )

    members = range(share)
    chips = range(kv_heads)
    slots = range(MOST)

    def relay_rows(j):
        arrived(kv_rn.at[0, j], r_rn.at[0, j])
        for k in range(1, share):
            start("rows", kv_rn.at[0, j], kv_rn.at[share - k, j], r_rn.at[share - k, j], b, peers[k])

    def peers_rows(j):
        for kk in range(1, share):
            arrived(kv_rn.at[kk, j], r_rn.at[kk, j])

    def relay_near(j):
        for k in range(near_count):
            arrived(kv_mov.at[k, 0, j], r_mov.at[k, j, 0])
            for p in range(1, share):
                start("pair", kv_mov.at[k, 0, j], kv_mov.at[k, share - p, j], r_peer.at[k, share - p - 1, j // 2], b, peers[p])

    def relay_far(e, j, m):
        i = near_count + e
        spot = kv_mov.at[i, 0, j, m]
        arrived(spot, r_mov.at[i, j, m])
        for p in range(1, share):
            start("page", spot, kv_mov.at[i, share - p, j, m], r_peer.at[i, share - p - 1, m], b, peers[p])

    def hub_relay(spots):
        @pl.when(is_hub)
        def _():
            for e, j in spots:
                i = near_count + e
                spot = kv_mov.at[i, 0, j, 1]
                arrived(spot, r_mov.at[i, j, 1])
                start("hub", spot, kv_mov.at[i, 0, j, 1], r_mov.at[i, j, 1], near(1), a)
                for p in range(1, share):
                    start("hub", spot, kv_mov.at[i, share - p, j, 1], r_peer.at[i, share - p - 1, 1], b, peers[p])

    def leaf_relay(spots):
        @pl.when(jnp.logical_not(is_hub))
        def _():
            for e, j in spots:
                i = near_count + e
                spot = kv_mov.at[i, 0, j, 1]
                arrived(spot, r_mov.at[i, j, 1])
                for p in range(1, share):
                    start("leaf", spot, kv_mov.at[i, share - p, j, 1], r_peer.at[i, share - p - 1, 1], b, peers[p])

    def send_metas():
        arrived(metas.at[0, 0, 1:kv_heads], r_meta.at[0, 0])
        block = metas.at[0, 0]
        for t in range(half):
            g = 1 + near_count + reach
            start("block", block, metas.at[g, 0], r_meta.at[g, 0], far(t), a)
        for k in range(1, half):
            start("block", block, metas.at[k, 0], r_meta.at[k, 0], near(k), a)
        for p in range(1, share):
            start("part", metas.at[0, 0, 1:kv_heads], metas.at[0, share - p, 1:kv_heads], r_meta.at[groups, share - p], b, peers[p])

    def relay_metas(lo, hi):
        for g in range(lo, hi):
            arrived(metas.at[g, 0], r_meta.at[g, 0])
            for p in range(1, share):
                start("block", metas.at[g, 0], metas.at[g, share - p], r_meta.at[lo, share - p], b, peers[p])

    def peers_own_row():
        for kk in range(1, share):
            arrived(metas.at[0, kk, 0], r_meta.at[0, kk])

    def peers_plane():
        for kk in range(1, share):
            arrived(metas.at[0, kk, 1:kv_heads], r_meta.at[groups, kk])

    def peers_metas(lo, hi):
        for kk in range(1, share):
            arrived(metas.at[lo:hi, kk], r_meta.at[lo, kk])

    def attend_near(part):
        js = list(chips)[2 * part:2 * part + 2]
        for k in range(near_count):
            attend_moved([(k, kk, j, m) for j in js for kk in members for m in slots])

    def peers_near(part):
        js = list(chips)[2 * part:2 * part + 2]
        for k in range(near_count):
            for kk in range(1, share):
                arrived(kv_mov.at[k, kk, js[0]:js[-1] + 1], r_peer.at[k, kk - 1, part])

    def peers_far(e, m):
        i = near_count + e
        for kk in range(1, share):
            arrived(kv_mov.at[i, kk, :, m], r_peer.at[i, kk - 1, m])

    def attend_far(e, m):
        attend_moved([(near_count + e, kk, j, m) for j in chips for kk in members])

    others = range(1, kv_heads)
    late = [m for m in reversed(slots) if m == 0 or not shared]

    def relay_late(j):
        for e in range(half):
            for m in late:
                relay_far(e, j, m)

    send_on(1, 0)
    send_on(2, 0)
    peers_own_row()
    peers_rows(0)
    attend_resident([(kk, 0) for kk in members], True)
    send_on(3, 0)
    send_metas()
    send_on(1, 1)
    send_on(2, 1)
    send_on(3, 1)
    first_far = 1 + near_count
    if shared:
        hub_relay([(0, 0), (1, 0), (0, 1)])
    if near_count:
        relay_metas(1, first_far)
    relay_near(0)
    relay_near(1)
    relay_late(0)
    if shared:
        hub_relay([(0, 2), (1, 1), (0, 3), (1, 2), (1, 3)])
    if near_count:
        peers_metas(1, first_far)
    peers_near(0)
    attend_near(0)
    relay_near(2)
    relay_near(3)
    relay_rows(1)
    relay_rows(2)
    peers_near(1)
    attend_near(1)
    relay_rows(3)
    relay_late(1)
    peers_plane()
    peers_rows(1)
    peers_rows(2)
    attend_resident([(kk, 1) for kk in members])
    attend_resident([(kk, 2) for kk in members])
    relay_late(2)
    relay_metas(first_far, groups)
    relay_late(3)
    if shared:
        leaf_relay([(0, j) for j in chips])
    peers_rows(3)
    attend_resident([(kk, 3) for kk in members])
    attend_fresh()
    if shared:
        leaf_relay([(e, j) for e in range(1, half) for j in chips])
    peers_metas(first_far, groups)
    for e in range(half):
        for m in reversed(slots):
            peers_far(e, m)
        for m in reversed(slots):
            attend_far(e, m)

    def turn(h):
        part = slice(h * queries, (h + 1) * queries)
        return (run_out[:, part] / run_sum[:, part]).T

    for h in range(heads):
        out_ref[:, h * HEAD_DIM:(h + 1) * HEAD_DIM] = turn(h).astype(out_ref.dtype)

    for name in names:
        if name not in ("hub", "leaf"):
            all_left(name)
    for src, j, part in wide:
        remote(src, src, s_wide.at[j, part], s_load.at[0], b, a).wait_send()
    if shared:
        @pl.when(is_hub)
        def _():
            all_left("hub")

        @pl.when(jnp.logical_not(is_hub))
        def _():
            all_left("leaf")


def finish(append_ref, rows_ref, pool_ref, fresh_ref, out_ref, updated_ref):
    out_ref[...] = rows_ref[...]
    updated_ref[...] = pool_ref[...]
    updated_ref[append_ref[0, 0], 0:fresh_ref.shape[0]] = fresh_ref[...]


def local(n_inst, n_aa, queries, new_kv, pool, page_table, ctx_len, move_page, move_dest, append_page):
    pool_pages = pool[0]
    pages, page_rows, _, width = pool_pages.shape
    kv_heads = width // HEAD_DIM
    share = n_aa // kv_heads
    fresh_rows = new_kv[0]
    fresh_count = fresh_rows.shape[0]
    query_count, q_width = queries.shape[1:]
    heads = q_width // HEAD_DIM
    table = page_table.shape[1]
    moves = move_page.shape[1]
    half = n_inst // 2
    near = half - 1
    groups = 1 + near + half
    out_count = (near + half) * MOST
    per_kind = 2 if share < 4 else 9
    bf, f32 = jnp.bfloat16, jnp.float32
    dma = pltpu.SemaphoreType.DMA
    page = (2, page_rows, HEAD_DIM)
    rows = (2, fresh_count + table * page_rows, HEAD_DIM)
    attended = pl.pallas_call(
        functools.partial(kernel, n_inst, n_aa, kv_heads),
        out_shape=pltpu.VMEM((query_count, q_width), bf),
        in_specs=[pl.BlockSpec(memory_space=pltpu.HBM)] * 7,
        out_specs=pl.BlockSpec(memory_space=pltpu.VMEM),
        scratch_shapes=[
            *[pltpu.SMEM(x.shape, jnp.int32) for x in (page_table, ctx_len, move_page, move_dest)],
            pltpu.VMEM((query_count, q_width), bf),
            pltpu.VMEM(pool_pages.shape, bf),
            pltpu.VMEM(fresh_rows.shape, bf),
            pltpu.VMEM((moves, kv_heads, *page), bf),
            pltpu.VMEM((kv_heads, *rows), bf),
            pltpu.VMEM((kv_heads * out_count, *page), bf),
            pltpu.VMEM((kv_heads, out_count, *page), bf),
            pltpu.VMEM((near + half, share, kv_heads, MOST, *page), bf),
            pltpu.VMEM((share, kv_heads, *rows), bf),
            pltpu.VMEM((groups, share, kv_heads, 1, LANES), jnp.int32),
            pltpu.VMEM((1, heads * query_count), f32),
            pltpu.VMEM((1, heads * query_count), f32),
            pltpu.VMEM((1, heads * query_count), f32),
            pltpu.VMEM((HEAD_DIM, heads * query_count), f32),
            pltpu.VMEM((2 * HEAD_DIM, heads * query_count), bf),
            dma((7,)), dma((8, per_kind)),
            dma((share, kv_heads)), dma((near + half, kv_heads, MOST)), dma((near + half, share - 1, MOST)),
            dma((kv_heads, 2)), dma((groups + 1, share)), dma((kv_heads, 2) if half > 2 else (1, 1)),
        ],
        compiler_params=pltpu.CompilerParams(collective_id=0, has_side_effects=True, vmem_limit_bytes=60 * 2**20),
        name="paged_attention",
    )(page_table, ctx_len, move_page, move_dest, queries[0], pool_pages, fresh_rows)
    attended, updated = pl.pallas_call(
        finish,
        out_shape=(
            jax.ShapeDtypeStruct(attended.shape, bf),
            jax.ShapeDtypeStruct(pool_pages.shape, bf),
        ),
        in_specs=[pl.BlockSpec(memory_space=pltpu.SMEM)] + [pl.BlockSpec(memory_space=pltpu.VMEM)] * 3,
        out_specs=(pl.BlockSpec(memory_space=pltpu.VMEM),) * 2,
        compiler_params=pltpu.CompilerParams(vmem_limit_bytes=12 * 2**20),
        name="finish",
    )(append_page, attended, pool_pages, fresh_rows)
    return (attended[None], updated[None])


def solution(mesh):
    return jax.shard_map(
        functools.partial(local, mesh.shape["ba"], mesh.shape["aa"]),
        mesh=mesh,
        in_specs=(
            P("ba", None, "aa"),
            P("ba", "aa", None, None),
            P("ba", "aa", None, None, None),
            P("ba", "aa"),
            P("ba", "aa"),
            P("ba", "aa"),
            P("ba", "aa"),
            P("ba", "aa"),
        ),
        out_specs=(P("ba", None, "aa"), P("ba", "aa", None, None, None)),
        check_vma=False,
    )
```
